32 devices in a mesh: dp: 4 (over y, z), tp: 8 (over x, core).
Axes of the slice: x: 4, y: 2, z: 2, core: 2. Of those that a mesh axis runs over, the one named last changes fastest.
The devices are a block of a 4x4x8 slice.
Arguments:
- hidden: bfloat16 [512, 4096], P('dp'), parts along dimension 0
- w_gate: bfloat16 [4096, 14336], P(None, 'tp')
- w_up: bfloat16 [4096, 14336], P(None, 'tp')
- w_down: bfloat16 [14336, 4096], P('tp')
- norm_gain: float32 [4096], replicated
- w_vocab: bfloat16 [4096, 32768], P(None, 'tp')
- temperature: float32 [512], P('dp'), parts along dimension 0
- target: int32 [512], P('dp'), parts along dimension 0
Outputs:
- output 1: float32 [512], P('dp'), parts along dimension 0
- output 2: float32 [512], P('dp'), parts along dimension 0
- output 3: float32 [512], P('dp'), parts along dimension 0
- output 4: bfloat16 [512, 32768], P('dp'), parts along dimension 0
There are 4 independent parts. The reference program is written for one: setup_inputs(seed, part) draws one part's arguments, and reference() takes and returns one part's arrays. A program takes and returns all parts, laid end to end along the dimension named above; an argument that names none is the same for every part.
All inputs are finite; a program needn't handle non-finite values.
Results may differ from the reference program's by a relative error of at most 0.00436137.
Values are sent between devices in bfloat16 or wider.
A program may use at most 768 MiB of HBM per device.

```python
import jax
import jax.numpy as jnp
from jax import lax

MODEL_DIM = 4096
FF_DIM = 14336
VOCAB_SIZE = 32768
BATCH_ROWS = 128
ROW_BLOCK = min(32, BATCH_ROWS)
NORM_EPS = 1e-6


def setup_inputs(seed: int = 0, part: int = 0) -> dict:
    shared_keys = jax.random.split(jax.random.key(seed), 5)
    part_keys = jax.random.split(jax.random.fold_in(jax.random.key(seed + 1), part), 3)
    hidden = jax.random.normal(part_keys[0], (BATCH_ROWS, MODEL_DIM), jnp.float32)
    w_gate = jax.random.normal(shared_keys[0], (MODEL_DIM, FF_DIM), jnp.float32) * MODEL_DIM ** -0.5
    w_up = jax.random.normal(shared_keys[1], (MODEL_DIM, FF_DIM), jnp.float32) * MODEL_DIM ** -0.5
    w_down = jax.random.normal(shared_keys[2], (FF_DIM, MODEL_DIM), jnp.float32) * (2.0 * FF_DIM ** -0.5)
    norm_gain = jax.random.uniform(shared_keys[3], (MODEL_DIM,), jnp.float32, 0.5, 1.5)
    w_vocab = jax.random.normal(shared_keys[4], (MODEL_DIM, VOCAB_SIZE), jnp.float32) * (1.5 * MODEL_DIM ** -0.5)
    temperature = jax.random.uniform(part_keys[1], (BATCH_ROWS,), jnp.float32, 0.5, 2.0)
    target = jax.random.randint(part_keys[2], (BATCH_ROWS,), 0, VOCAB_SIZE, jnp.int32)
    return {
        "hidden": hidden.astype(jnp.bfloat16),
        "w_gate": w_gate.astype(jnp.bfloat16),
        "w_up": w_up.astype(jnp.bfloat16),
        "w_down": w_down.astype(jnp.bfloat16),
        "norm_gain": norm_gain,
        "w_vocab": w_vocab.astype(jnp.bfloat16),
        "temperature": temperature,
        "target": target,
    }


def reference(hidden, w_gate, w_up, w_down, norm_gain, w_vocab, temperature, target):
    block_count = hidden.shape[0] // ROW_BLOCK
    hidden_blocks = hidden.reshape(block_count, ROW_BLOCK, hidden.shape[1])
    temp_blocks = temperature.reshape(block_count, ROW_BLOCK)
    target_blocks = target.reshape(block_count, ROW_BLOCK)
    vocab_ids = jnp.arange(w_vocab.shape[1], dtype=jnp.int32)

    def one_block(block):
        hidden_rows, temp_rows, target_rows = block
        gate_pre = jnp.dot(hidden_rows, w_gate, preferred_element_type=jnp.float32)
        up_pre = jnp.dot(hidden_rows, w_up, preferred_element_type=jnp.float32)
        hidden_act = (jax.nn.silu(gate_pre) * up_pre).astype(jnp.bfloat16)
        mlp_out = jnp.dot(hidden_act, w_down, preferred_element_type=jnp.float32)
        residual = hidden_rows.astype(jnp.float32) + mlp_out
        inv_rms = lax.rsqrt(jnp.mean(residual * residual, axis=-1, keepdims=True) + NORM_EPS)
        normed = (norm_gain * residual * inv_rms).astype(jnp.bfloat16)
        logits = jnp.dot(normed, w_vocab, preferred_element_type=jnp.float32) / temp_rows[:, None]
        row_max = jnp.max(logits, axis=-1, keepdims=True)
        shifted = jnp.exp(logits - row_max)
        sum_exp = jnp.sum(shifted, axis=-1)
        log_norm = row_max[:, 0] + jnp.log(sum_exp)
        entropy = log_norm - jnp.sum(shifted * logits, axis=-1) / sum_exp
        target_logit = jnp.sum(jnp.where(vocab_ids[None, :] == target_rows[:, None], logits, 0.0), axis=-1)
        log_probs = (logits - log_norm[:, None]).astype(jnp.bfloat16)
        return log_norm, entropy, target_logit - log_norm, log_probs

    log_norm, entropy, target_logp, log_probs = lax.map(one_block, (hidden_blocks, temp_blocks, target_blocks))
    return (
        log_norm.reshape(-1),
        entropy.reshape(-1),
        target_logp.reshape(-1),
        log_probs.reshape(-1, w_vocab.shape[1]),
    )
```

```python
import functools

import jax
import jax.numpy as jnp
from jax import lax
from jax.experimental import pallas as pl
from jax.experimental.pallas import tpu as pltpu
from jax.sharding import PartitionSpec as P

NORM_EPS = 1e-6
MESH = pl.DeviceIdType.MESH
F32 = jnp.float32
BF16 = jnp.bfloat16

SLAB = 256
AHEAD = 3

ID_PART = 0
ID_ATOP, ID_ABOT, ID_BNXT, ID_BPRV = 4, 5, 6, 7
ID_YNXT, ID_YPRV, ID_YDIE = 8, 9, 10
ID_RNXT, ID_RPRV = 11, 12
ID_FPRV, ID_FNXT, ID_FTOP, ID_FBOT = 13, 14, 15, 16
ID_ZNXT = 17


def main_kernel(n, h_hbm, wg_hbm, wu_hbm, wd_hbm, gain_hbm, wv_hbm, temp_hbm, targ_hbm,
                z_ref, st_ref,
                wbuf, dbuf, h_ref, x_ref, a_ref, gain_ref, temp_ref, targ_ref,
                psend, prcv, abuf, arcv, bsend, brcv, chip_ref, ygat, cols_ref,
                ss, rs, wsem, dsem, msem):
    chips = n // 2
    rows, dim = h_ref.shape
    half = rows // 2
    f_loc = a_ref.shape[1]
    nf = f_loc // SLAB
    own_w = dim // n
    tile_w = z_ref.shape[2]
    tiles = z_ref.shape[0] // n
    per_tile = tile_w // SLAB
    id_zprv = ID_ZNXT + tiles
    id_zdie = id_zprv + tiles
    id_zrel = id_zdie + tiles
    id_zfp = id_zrel + tiles
    id_zfn = id_zfp + tiles
    id_zfo = id_zfn + tiles
    id_stat = id_zfo + tiles

    me = lax.axis_index("tp")
    chip, core = me // 2, me % 2
    other = 1 - core
    c_nxt, c_prv, c_opp = (chip + 1) % chips, (chip + chips - 1) % chips, (chip + 2) % chips
    nxt, prv, opp = c_nxt * 2 + core, c_prv * 2 + core, c_opp * 2 + core
    die = chip * 2 + other

    def remote(src, dst, k, dev):
        return pltpu.make_async_remote_copy(src_ref=src, dst_ref=dst, send_sem=ss.at[k], recv_sem=rs.at[k],
                                            device_id={"tp": dev}, device_id_type=MESH)

    small = [pltpu.make_async_copy(h_hbm, h_ref, msem.at[0]),
             pltpu.make_async_copy(gain_hbm, gain_ref, msem.at[1]),
             pltpu.make_async_copy(temp_hbm, temp_ref, msem.at[2]),
             pltpu.make_async_copy(targ_hbm, targ_ref, msem.at[3])]

    def gate_up(j):
        col = pl.ds(pl.multiple_of(j * SLAB, SLAB), SLAB)
        return (pltpu.make_async_copy(wg_hbm.at[:, col], wbuf.at[2 * j], wsem.at[2 * j]),
                pltpu.make_async_copy(wu_hbm.at[:, col], wbuf.at[2 * j + 1], wsem.at[2 * j + 1]))

    def vocab(s):
        col = pl.ds(pl.multiple_of(s * SLAB, SLAB), SLAB)
        return pltpu.make_async_copy(wv_hbm.at[:, col], wbuf.at[s], wsem.at[s])

    def down(k, dev):
        col = pl.ds(pl.multiple_of(dev * own_w, own_w), own_w)
        return pltpu.make_async_copy(wd_hbm.at[:, col], dbuf.at[k], dsem.at[k])

    order = []
    for target in (c_opp, c_nxt, c_prv, chip):
        order += [target * 2 + other, target * 2 + core]

    small[0].start()
    for j in range(AHEAD):
        for c in gate_up(j):
            c.start()
    for c in small[1:]:
        c.start()

    barrier = pltpu.get_barrier_semaphore()
    for r in range(1, n):
        pl.semaphore_signal(barrier, inc=1, device_id={"tp": (me + r) % n}, device_id_type=MESH)

    small[0].wait()

    @pl.loop(0, nf)
    def _(j):
        for c in gate_up(j):
            c.wait()

        @pl.when(j + AHEAD < nf)
        def _():
            for c in gate_up(j + AHEAD):
                c.start()

        @pl.when(j + AHEAD >= nf)
        def _():
            for k in range(AHEAD):
                @pl.when(j + AHEAD == nf + k)
                def _():
                    down(k, order[k]).start()

        gate = jnp.dot(h_ref[...], wbuf[2 * j], preferred_element_type=F32)
        up = jnp.dot(h_ref[...], wbuf[2 * j + 1], preferred_element_type=F32)
        a_ref[:, pl.ds(pl.multiple_of(j * SLAB, SLAB), SLAB)] = (jax.nn.silu(gate) * up).astype(BF16)

    for c in small[1:]:
        c.wait()
    row_ids = lax.broadcasted_iota(jnp.int32, (rows, rows), 0)
    lane_ids = lax.broadcasted_iota(jnp.int32, (rows, rows), 1)
    eye = row_ids == lane_ids
    inv_temp = 1.0 / jnp.sum(jnp.where(eye, temp_ref[...], 0.0), axis=1, keepdims=True)
    targ = jnp.sum(jnp.where(eye, targ_ref[...].astype(F32), 0.0), axis=1, keepdims=True)
    cols_ref[0] = jnp.broadcast_to(inv_temp, (rows, 128))
    cols_ref[1] = jnp.broadcast_to(targ, (rows, 128))

    pl.semaphore_wait(barrier, n - 1)

    copies = []
    for k in range(2 * chips):
        if k + AHEAD < 2 * chips:
            down(k + AHEAD, order[k + AHEAD]).start()
        else:
            per = (tiles * per_tile) // AHEAD
            first = (k + AHEAD - 2 * chips) * per
            last = tiles * per_tile if k == 2 * chips - 1 else first + per
            for s in range(first, last):
                vocab(s).start()
        down(k, order[k]).wait()
        part = jnp.dot(a_ref[...], dbuf[k], preferred_element_type=F32)
        q = k // 2
        to_die = remote(psend.at[q], prcv.at[q], ID_PART + q, die)
        if k % 2 == 0:
            psend[q] = part.astype(BF16)
            to_die.start()
            copies.append(to_die)
            continue
        to_die.wait_recv()
        total = part + prcv[q].astype(F32)
        if q == 0:
            abuf[...] = total.astype(BF16)
            top = remote(abuf.at[pl.ds(0, half)], arcv.at[0], ID_ATOP, nxt)
            bot = remote(abuf.at[pl.ds(half, half)], arcv.at[1], ID_ABOT, prv)
            top.start()
            bot.start()
            copies += [top, bot]
        elif q < 3:
            chip_ref[q - 1] = total
        if q == 2:
            top.wait_recv()
            bsend[0, :half] = (chip_ref[0, :half] + arcv[0].astype(F32)).astype(BF16)
            bsend[0, half:] = chip_ref[0, half:].astype(BF16)
            b_nxt = remote(bsend.at[0], brcv.at[0], ID_BNXT, nxt)
            b_nxt.start()
            bot.wait_recv()
            bsend[1, :half] = chip_ref[1, :half].astype(BF16)
            bsend[1, half:] = (chip_ref[1, half:] + arcv[1].astype(F32)).astype(BF16)
            b_prv = remote(bsend.at[1], brcv.at[1], ID_BPRV, prv)
            b_prv.start()
            copies += [b_nxt, b_prv]
    b_nxt.wait_recv()
    b_prv.wait_recv()
    ygat[me] = (total + brcv[0].astype(F32) + brcv[1].astype(F32)).astype(BF16)

    y_nxt = remote(ygat.at[me], ygat.at[me], ID_YNXT, nxt)
    y_prv = remote(ygat.at[me], ygat.at[me], ID_YPRV, prv)
    y_die = remote(ygat.at[me], ygat.at[me], ID_YDIE, die)
    for c in (y_nxt, y_prv, y_die):
        c.start()
    top_rows, bot_rows = pl.ds(0, half), pl.ds(half, half)
    remote(ygat.at[prv], ygat.at[prv], ID_YNXT, nxt).wait_recv()
    r_nxt = remote(ygat.at[prv, top_rows], ygat.at[prv, top_rows], ID_RNXT, nxt)
    f_prv = remote(ygat.at[prv], ygat.at[prv], ID_FPRV, die)
    r_nxt.start()
    f_prv.start()
    remote(ygat.at[nxt], ygat.at[nxt], ID_YPRV, prv).wait_recv()
    r_prv = remote(ygat.at[nxt, bot_rows], ygat.at[nxt, bot_rows], ID_RPRV, prv)
    f_nxt = remote(ygat.at[nxt], ygat.at[nxt], ID_FNXT, die)
    r_prv.start()
    f_nxt.start()

    def residual(s):
        col = pl.ds(pl.multiple_of(s * own_w, own_w), own_w)
        return col, h_ref[:, col].astype(F32) + ygat[s].astype(F32)

    def squares(s):
        _, r = residual(s)
        return jnp.sum(r * r, axis=1, keepdims=True)

    total_sq = squares(me) + squares(prv) + squares(nxt)
    remote(ygat.at[die], ygat.at[die], ID_YDIE, die).wait_recv()
    total_sq += squares(die)
    p_prv, p_nxt, p_opp = c_prv * 2 + other, c_nxt * 2 + other, c_opp * 2 + other
    remote(ygat.at[p_prv], ygat.at[p_prv], ID_FPRV, die).wait_recv()
    total_sq += squares(p_prv)
    remote(ygat.at[p_nxt], ygat.at[p_nxt], ID_FNXT, die).wait_recv()
    total_sq += squares(p_nxt)
    remote(ygat.at[opp, top_rows], ygat.at[opp, top_rows], ID_RNXT, nxt).wait_recv()
    f_top = remote(ygat.at[opp, top_rows], ygat.at[opp, top_rows], ID_FTOP, die)
    f_top.start()
    remote(ygat.at[opp, bot_rows], ygat.at[opp, bot_rows], ID_RPRV, prv).wait_recv()
    f_bot = remote(ygat.at[opp, bot_rows], ygat.at[opp, bot_rows], ID_FBOT, die)
    f_bot.start()
    total_sq += squares(opp)
    remote(ygat.at[p_opp, top_rows], ygat.at[p_opp, top_rows], ID_FTOP, die).wait_recv()
    remote(ygat.at[p_opp, bot_rows], ygat.at[p_opp, bot_rows], ID_FBOT, die).wait_recv()
    total_sq += squares(p_opp)
    copies += [y_nxt, y_prv, y_die, r_nxt, r_prv, f_prv, f_nxt, f_top, f_bot]
    inv_rms = lax.rsqrt(total_sq * (1.0 / dim) + NORM_EPS)

    @pl.loop(0, n)
    def _(s):
        col, r = residual(s)
        x_ref[:, col] = (gain_ref[:, col] * r * inv_rms).astype(BF16)

    cols_ref[2] = jnp.zeros((rows, 128), F32)
    lanes = lax.broadcasted_iota(jnp.int32, (rows, 128), 1)

    def own_sends(t):
        blk = z_ref.at[me * tiles + t]
        return (remote(blk, blk, ID_ZNXT + t, nxt), remote(blk, blk, id_zprv + t, prv),
                remote(blk, blk, id_zdie + t, die))

    @pl.loop(0, tiles)
    def _(t):
        for i in range(per_tile):
            vocab(t * per_tile + i).wait()
        pieces = [jnp.dot(x_ref[...], wbuf[t * per_tile + i], preferred_element_type=F32) for i in range(per_tile)]
        logits = jnp.concatenate(pieces, axis=1) * cols_ref[0][:, :1]
        top_l = jnp.max(logits, axis=1, keepdims=True)
        low = logits - top_l
        z_ref[me * tiles + t] = low.astype(BF16)
        for c in own_sends(t):
            c.start()
        e = jnp.exp(low)
        ids = lax.broadcasted_iota(jnp.int32, (rows, tile_w), 1) + (me * tiles + t) * tile_w
        hit = jnp.where(ids.astype(F32) == cols_ref[1][:, :1], logits, 0.0)
        stats = cols_ref[2]
        for i, col in enumerate((top_l, jnp.sum(e, axis=1, keepdims=True), jnp.sum(e * logits, axis=1, keepdims=True),
                                 jnp.sum(hit, axis=1, keepdims=True))):
            stats = jnp.where(lanes == i * tiles + t, col, stats)
        cols_ref[2] = stats

    st_ref[me] = cols_ref[2].T[:4 * tiles]
    stat_sends = [remote(st_ref.at[me], st_ref.at[me], id_stat + r - 1, (me + r) % n) for r in range(1, n)]
    for c in stat_sends:
        c.start()
    copies += stat_sends

    def blk(dev, t):
        return z_ref.at[dev * tiles + t]

    for t in range(tiles):
        copies += own_sends(t)
        remote(blk(prv, t), blk(prv, t), ID_ZNXT + t, nxt).wait_recv()
        if t % 2 == 0:
            rel = remote(blk(prv, t), blk(prv, t), id_zrel + t, nxt)
            rel.start()
            copies.append(rel)
        fwd = remote(blk(prv, t), blk(prv, t), id_zfp + t, die)
        fwd.start()
        copies.append(fwd)
        remote(blk(nxt, t), blk(nxt, t), id_zprv + t, prv).wait_recv()
        if t % 2 == 1:
            rel = remote(blk(nxt, t), blk(nxt, t), id_zrel + t, prv)
            rel.start()
            copies.append(rel)
        fwd = remote(blk(nxt, t), blk(nxt, t), id_zfn + t, die)
        fwd.start()
        copies.append(fwd)
    for t in range(tiles):
        remote(blk(opp, t), blk(opp, t), id_zrel + t, nxt if t % 2 == 0 else prv).wait_recv()
        fwd = remote(blk(opp, t), blk(opp, t), id_zfo + t, die)
        fwd.start()
        copies.append(fwd)
    for t in range(tiles):
        remote(blk(die, t), blk(die, t), id_zdie + t, die).wait_recv()
        remote(blk(p_prv, t), blk(p_prv, t), id_zfp + t, die).wait_recv()
        remote(blk(p_nxt, t), blk(p_nxt, t), id_zfn + t, die).wait_recv()
    for t in range(tiles):
        remote(blk(p_opp, t), blk(p_opp, t), id_zfo + t, die).wait_recv()
    for r in range(1, n):
        src = (me + n - r) % n
        remote(st_ref.at[src], st_ref.at[src], id_stat + r - 1, src).wait_recv()
    for c in copies:
        c.wait_send()


def finish_kernel(z_ref, st_ref, norm_ref, ent_ref, logp_ref, out_hbm, d_ref, obuf, sem):
    blocks, rows, width = z_ref.shape
    n, four_t, _ = st_ref.shape
    tiles = four_t // 4
    top = jnp.max(jnp.max(st_ref[:, :tiles], axis=0), axis=0, keepdims=True)
    scale = jnp.exp(st_ref[:, :tiles] - top[None])

    def total(v):
        return jnp.sum(jnp.sum(v, axis=0), axis=0, keepdims=True)

    sum_exp = total(st_ref[:, tiles:2 * tiles] * scale)
    weighted = total(st_ref[:, 2 * tiles:3 * tiles] * scale)
    target_logit = total(st_ref[:, 3 * tiles:])
    log_norm = top + jnp.log(sum_exp)
    norm_ref[...] = log_norm
    ent_ref[...] = log_norm - weighted / sum_exp
    logp_ref[...] = target_logit - log_norm
    for dev in range(n):
        d_ref[dev] = jnp.concatenate([st_ref[dev, :tiles] - log_norm,
                                      jnp.zeros((128 - tiles, rows), F32)], axis=0).T

    def put(dev, t):
        b = dev * tiles + t
        return pltpu.make_async_copy(
            obuf.at[b], out_hbm.at[:, pl.ds(pl.multiple_of(b * width, width), width)], sem.at[b])

    @pl.loop(0, n)
    def _(dev):
        shift = d_ref[dev]
        for t in range(tiles):
            obuf[dev * tiles + t] = (z_ref[dev * tiles + t].astype(F32) + shift[:, t:t + 1]).astype(BF16)
            put(dev, t).start()

    @pl.loop(0, n)
    def _(dev):
        for t in range(tiles):
            put(dev, t).wait()


def solution(mesh):
    n = mesh.shape["tp"]

    def device_step(hidden, w_gate, w_up, w_down, norm_gain, w_vocab, temperature, target):
        rows, dim = hidden.shape
        f_loc = w_gate.shape[1]
        v_loc = w_vocab.shape[1]
        own_w = dim // n
        tile_w = 512
        tiles = v_loc // tile_w
        n_ids = ID_ZNXT + 7 * tiles + n
        any_spec = pl.BlockSpec(memory_space=pl.ANY)
        vmem = pl.BlockSpec(memory_space=pltpu.VMEM)
        z, stats = pl.pallas_call(
            functools.partial(main_kernel, n),
            out_shape=(pltpu.VMEM((n * tiles, rows, tile_w), BF16), pltpu.VMEM((n, 4 * tiles, rows), F32)),
            in_specs=[any_spec] * 8,
            out_specs=(vmem, vmem),
            scratch_shapes=[
                pltpu.VMEM((v_loc // SLAB, dim, SLAB), BF16),
                pltpu.VMEM((n, f_loc, own_w), BF16),
                pltpu.VMEM((rows, dim), BF16),
                pltpu.VMEM((rows, dim), BF16),
                pltpu.VMEM((rows, f_loc), BF16),
                pltpu.VMEM((1, dim), F32),
                pltpu.VMEM((1, rows), F32),
                pltpu.VMEM((1, rows), jnp.int32),
                pltpu.VMEM((4, rows, own_w), BF16),
                pltpu.VMEM((4, rows, own_w), BF16),
                pltpu.VMEM((rows, own_w), BF16),
                pltpu.VMEM((2, rows // 2, own_w), BF16),
                pltpu.VMEM((2, rows, own_w), BF16),
                pltpu.VMEM((2, rows, own_w), BF16),
                pltpu.VMEM((2, rows, own_w), F32),
                pltpu.VMEM((n, rows, own_w), BF16),
                pltpu.VMEM((3, rows, 128), F32),
                pltpu.SemaphoreType.DMA((n_ids,)),
                pltpu.SemaphoreType.DMA((n_ids,)),
                pltpu.SemaphoreType.DMA((v_loc // SLAB,)),
                pltpu.SemaphoreType.DMA((n,)),
                pltpu.SemaphoreType.DMA((4,)),
            ],
            compiler_params=pltpu.CompilerParams(
                collective_id=0, has_side_effects=True, vmem_limit_bytes=55 * 1024 * 1024),
            name="decode_tail",
        )(hidden, w_gate, w_up, w_down, norm_gain.reshape(1, dim), w_vocab, temperature.reshape(1, rows),
          target.reshape(1, rows))
        row = jax.ShapeDtypeStruct((1, rows), F32)
        log_norm, entropy, target_logp, log_probs = pl.pallas_call(
            finish_kernel,
            out_shape=(row, row, row, jax.ShapeDtypeStruct((rows, n * v_loc), BF16)),
            in_specs=[vmem, vmem],
            out_specs=(vmem, vmem, vmem, any_spec),
            scratch_shapes=[
                pltpu.VMEM((n, rows, 128), F32),
                pltpu.VMEM((n * tiles, rows, tile_w), BF16),
                pltpu.SemaphoreType.DMA((n * tiles,)),
            ],
            compiler_params=pltpu.CompilerParams(vmem_limit_bytes=24 * 1024 * 1024),
            name="write_log_probs",
        )(z, stats)
        return log_norm.reshape(rows), entropy.reshape(rows), target_logp.reshape(rows), log_probs

    return jax.shard_map(
        device_step,
        mesh=mesh,
        in_specs=(P("dp", None), P(None, "tp"), P(None, "tp"), P("tp", None), P(None),
                  P(None, "tp"), P("dp"), P("dp")),
        out_specs=(P("dp"), P("dp"), P("dp"), P("dp", None)),
        check_vma=False,
    )
```

```python
import functools

import jax
import jax.numpy as jnp
from jax import lax
from jax.experimental import pallas as pl
from jax.experimental.pallas import tpu as pltpu
from jax.sharding import PartitionSpec as P

NORM_EPS = 1e-6
MESH = pl.DeviceIdType.MESH
F32 = jnp.float32
BF16 = jnp.bfloat16

SLAB = 256
AHEAD = 3
DOWN_AHEAD = 3
DOWN_SLOTS = 5
GROUPS = 2
TILE = 512
EARLY = 4


class Ids:
    def __init__(self, chips, tiles):
        self.count = 0
        g = GROUPS
        self.part = self.take(chips)
        self.atop, self.abot, self.bnxt, self.bprv = (self.take(g) for _ in range(4))
        self.ynxt, self.yprv, self.ydie = (self.take(g) for _ in range(3))
        self.rnxt, self.rprv, self.fprv, self.fnxt, self.ftop, self.fbot = (self.take(g) for _ in range(6))
        self.znxt, self.zprv, self.zdie, self.zrel, self.zfp, self.zfn, self.zfo = (
            self.take(g * tiles) for _ in range(7))
        self.snxt, self.sprv, self.sopp, self.sdie, self.sfp, self.sfn, self.sfo = (self.take(1) for _ in range(7))

    def take(self, k):
        first = self.count
        self.count += k
        return first


def main_kernel(n, h_hbm, wg_hbm, wu_hbm, wd_hbm, gain_hbm, wv_hbm, temp_hbm, targ_hbm,
                z_ref, fin_ref,
                wbuf, dbuf, h_ref, x_ref, a_ref, gain_ref, temp_ref, targ_ref,
                psend, prcv, abuf, arcv, bsend, brcv, chip_ref, ygat, cols_ref, st_ref, shift_ref,
                ss, rs, wsem, dsem, msem):
    chips = n // 2
    rows, dim = h_ref.shape
    grp = rows // GROUPS
    half = grp // 2
    kh = dim // 2
    f_loc = a_ref.shape[1]
    nf = f_loc // SLAB
    own_w = dim // n
    tiles = z_ref.shape[0] // n
    per_tile = TILE // SLAB
    ids = Ids(chips, tiles)

    me = lax.axis_index("tp")
    chip, core = me // 2, me % 2
    other = 1 - core
    c_nxt, c_prv, c_opp = (chip + 1) % chips, (chip + chips - 1) % chips, (chip + 2) % chips
    nxt, prv, opp = c_nxt * 2 + core, c_prv * 2 + core, c_opp * 2 + core
    die = chip * 2 + other
    p_prv, p_nxt, p_opp = c_prv * 2 + other, c_nxt * 2 + other, c_opp * 2 + other

    def remote(src, dst, k, dev):
        return pltpu.make_async_remote_copy(src_ref=src, dst_ref=dst, send_sem=ss.at[k], recv_sem=rs.at[k],
                                            device_id={"tp": dev}, device_id_type=MESH)

    copies = []

    def send(ref, k, dev):
        c = remote(ref, ref, k, dev)
        c.start()
        copies.append(c)
        return c

    def arrived(ref, k):
        remote(ref, ref, k, die).wait_recv()

    def g_rows(g):
        return pl.ds(g * grp, grp)

    def g_top(g):
        return pl.ds(g * grp, half)

    def g_bot(g):
        return pl.ds(g * grp + half, half)

    small = [pltpu.make_async_copy(h_hbm, h_ref, msem.at[0]),
             pltpu.make_async_copy(gain_hbm, gain_ref, msem.at[1]),
             pltpu.make_async_copy(temp_hbm, temp_ref, msem.at[2]),
             pltpu.make_async_copy(targ_hbm, targ_ref, msem.at[3])]

    def gate_up(j, part):
        col = pl.ds(pl.multiple_of(j * SLAB, SLAB), SLAB)
        k = pl.ds(part * kh, kh)
        return (pltpu.make_async_copy(wg_hbm.at[k, col], wbuf.at[2 * j, k], wsem.at[2 * part, j]),
                pltpu.make_async_copy(wu_hbm.at[k, col], wbuf.at[2 * j + 1, k], wsem.at[2 * part + 1, j]))

    def start_gate_up(j):
        for part in range(2):
            for c in gate_up(j, part):
                c.start()

    def vocab(s):
        col = pl.ds(pl.multiple_of(s * SLAB, SLAB), SLAB)
        return pltpu.make_async_copy(wv_hbm.at[:, col], wbuf.at[s], wsem.at[4, s])

    def down(k, dev):
        col = pl.ds(pl.multiple_of(dev * own_w, own_w), own_w)
        return pltpu.make_async_copy(wd_hbm.at[:, col], dbuf.at[k % DOWN_SLOTS], dsem.at[k])

    plan = ((c_opp, 0, True), (c_nxt, 1, True), (c_opp, 0, False), (c_prv, 2, True),
            (c_nxt, 1, False), (chip, 3, True), (c_prv, 2, False), (chip, 3, False))
    order = [c * 2 + (other if away else core) for c, _, away in plan]

    small[0].start()
    for j in range(AHEAD):
        start_gate_up(j)
    for c in small[1:]:
        c.start()

    barrier = pltpu.get_barrier_semaphore()
    for r in range(1, n):
        pl.semaphore_signal(barrier, inc=1, device_id={"tp": (me + r) % n}, device_id_type=MESH)

    small[0].wait()

    @pl.loop(0, nf)
    def _(j):
        for c in gate_up(j, 0):
            c.wait()

        @pl.when(j + AHEAD < nf)
        def _():
            start_gate_up(j + AHEAD)

        for k in range(DOWN_AHEAD):
            @pl.when(j == nf - AHEAD + min(k, AHEAD - 1))
            def _():
                down(k, order[k]).start()

        h0 = h_ref[:, :kh]
        gate = jnp.dot(h0, wbuf[2 * j, :kh], preferred_element_type=F32)
        up = jnp.dot(h0, wbuf[2 * j + 1, :kh], preferred_element_type=F32)
        for c in gate_up(j, 1):
            c.wait()
        h1 = h_ref[:, kh:]
        gate += jnp.dot(h1, wbuf[2 * j, kh:], preferred_element_type=F32)
        up += jnp.dot(h1, wbuf[2 * j + 1, kh:], preferred_element_type=F32)
        a_ref[:, pl.ds(pl.multiple_of(j * SLAB, SLAB), SLAB)] = (jax.nn.silu(gate) * up).astype(BF16)

    n_down = len(plan)
    for k, (_, q, away) in enumerate(plan):
        if k + DOWN_AHEAD < n_down:
            down(k + DOWN_AHEAD, order[k + DOWN_AHEAD]).start()
        else:
            per = (tiles * per_tile) // DOWN_AHEAD
            first = (k + DOWN_AHEAD - n_down) * per
            last = tiles * per_tile if k == n_down - 1 else first + per
            for s in range(first, last):
                vocab(s).start()
        down(k, order[k]).wait()
        part = jnp.dot(a_ref[...], dbuf[k % DOWN_SLOTS], preferred_element_type=F32)
        to_die = remote(psend.at[q], prcv.at[q], ids.part + q, die)
        if k == 0:
            pl.semaphore_wait(barrier, n - 1)
        if away:
            psend[q] = part.astype(BF16)
            to_die.start()
            copies.append(to_die)
            continue
        to_die.wait_recv()
        total = part + prcv[q].astype(F32)
        if q == 0:
            abuf[...] = total.astype(BF16)
            for g in range(GROUPS):
                for rws, k_id, dev in ((g_top(g), ids.atop, nxt), (g_bot(g), ids.abot, prv)):
                    c = remote(abuf.at[rws], arcv.at[rws], k_id + g, dev)
                    c.start()
                    copies.append(c)
        else:
            chip_ref[q - 1] = total

    for g in range(GROUPS):
        t_sl, b_sl = slice(g * grp, g * grp + half), slice(g * grp + half, (g + 1) * grp)
        arrived(arcv.at[g_top(g)], ids.atop + g)
        bsend[0, t_sl] = (chip_ref[0, t_sl] + arcv[t_sl].astype(F32)).astype(BF16)
        bsend[0, b_sl] = chip_ref[0, b_sl].astype(BF16)
        c = remote(bsend.at[0, g_rows(g)], brcv.at[0, g_rows(g)], ids.bnxt + g, nxt)
        c.start()
        copies.append(c)
        arrived(arcv.at[g_bot(g)], ids.abot + g)
        bsend[1, t_sl] = chip_ref[1, t_sl].astype(BF16)
        bsend[1, b_sl] = (chip_ref[1, b_sl] + arcv[b_sl].astype(F32)).astype(BF16)
        c = remote(bsend.at[1, g_rows(g)], brcv.at[1, g_rows(g)], ids.bprv + g, prv)
        c.start()
        copies.append(c)

    for c in small[1:]:
        c.wait()
    row_ids = lax.broadcasted_iota(jnp.int32, (rows, rows), 0)
    lane_ids = lax.broadcasted_iota(jnp.int32, (rows, rows), 1)
    eye = row_ids == lane_ids
    inv_temp = 1.0 / jnp.sum(jnp.where(eye, temp_ref[...], 0.0), axis=1, keepdims=True)
    targ = jnp.sum(jnp.where(eye, targ_ref[...].astype(F32), 0.0), axis=1, keepdims=True)
    cols_ref[0] = jnp.broadcast_to(inv_temp, (rows, 128))
    cols_ref[1] = jnp.broadcast_to(targ, (rows, 128))
    cols_ref[2] = jnp.zeros((rows, 128), F32)

    for g in range(GROUPS):
        g_sl = slice(g * grp, (g + 1) * grp)
        arrived(brcv.at[0, g_rows(g)], ids.bnxt + g)
        arrived(brcv.at[1, g_rows(g)], ids.bprv + g)
        ygat[me, g_sl] = (chip_ref[2, g_sl] + brcv[0, g_sl].astype(F32) + brcv[1, g_sl].astype(F32)).astype(BF16)
        own = ygat.at[me, g_rows(g)]
        send(own, ids.ynxt + g, nxt)
        send(own, ids.yprv + g, prv)
        send(own, ids.ydie + g, die)
    for g in range(GROUPS):
        arrived(ygat.at[prv, g_rows(g)], ids.ynxt + g)
        send(ygat.at[prv, g_top(g)], ids.rnxt + g, nxt)
        send(ygat.at[prv, g_rows(g)], ids.fprv + g, die)
        arrived(ygat.at[nxt, g_rows(g)], ids.yprv + g)
        send(ygat.at[nxt, g_bot(g)], ids.rprv + g, prv)
        send(ygat.at[nxt, g_rows(g)], ids.fnxt + g, die)

    def residual(s, g):
        col = pl.ds(pl.multiple_of(s * own_w, own_w), own_w)
        return col, h_ref[g_rows(g), col].astype(F32) + ygat[s, g * grp:(g + 1) * grp].astype(F32)

    def squares(s, g):
        _, r = residual(s, g)
        return jnp.sum(r * r, axis=1, keepdims=True)

    def finish_sum(g):
        arrived(ygat.at[opp, g_top(g)], ids.rnxt + g)
        send(ygat.at[opp, g_top(g)], ids.ftop + g, die)
        arrived(ygat.at[opp, g_bot(g)], ids.rprv + g)
        send(ygat.at[opp, g_bot(g)], ids.fbot + g, die)

    def normalize(g):
        total_sq = squares(me, g) + squares(prv, g) + squares(nxt, g) + squares(opp, g)
        for s, k in ((die, ids.ydie), (p_prv, ids.fprv), (p_nxt, ids.fnxt)):
            arrived(ygat.at[s, g_rows(g)], k + g)
            total_sq += squares(s, g)
        arrived(ygat.at[p_opp, g_top(g)], ids.ftop + g)
        arrived(ygat.at[p_opp, g_bot(g)], ids.fbot + g)
        total_sq += squares(p_opp, g)
        inv_rms = lax.rsqrt(total_sq * (1.0 / dim) + NORM_EPS)

        @pl.loop(0, n)
        def _(s):
            col, r = residual(s, g)
            x_ref[g_rows(g), col] = (gain_ref[:, col] * r * inv_rms).astype(BF16)

    lanes = lax.broadcasted_iota(jnp.int32, (grp, 128), 1)

    def blk(dev, t, g):
        return z_ref.at[dev * tiles + t, g_rows(g)]

    def own_sends(t, g):
        b = blk(me, t, g)
        at = g * tiles + t
        return (remote(b, b, ids.znxt + at, nxt), remote(b, b, ids.zprv + at, prv), remote(b, b, ids.zdie + at, die))

    def head(g, t0, t1):
        sl = slice(g * grp, (g + 1) * grp)

        @pl.loop(t0, t1)
        def _(t):
            if g == 0:
                for i in range(per_tile):
                    vocab(t * per_tile + i).wait()
            pieces = [jnp.dot(x_ref[sl], wbuf[t * per_tile + i], preferred_element_type=F32) for i in range(per_tile)]
            logits = jnp.concatenate(pieces, axis=1) * cols_ref[0, sl][:, :1]
            top_l = jnp.max(logits, axis=1, keepdims=True)
            low = logits - top_l
            z_ref[me * tiles + t, sl] = low.astype(BF16)
            for c in own_sends(t, g):
                c.start()
            e = jnp.exp(low)
            col_ids = lax.broadcasted_iota(jnp.int32, (grp, TILE), 1) + (me * tiles + t) * TILE
            hit = jnp.where(col_ids.astype(F32) == cols_ref[1, sl][:, :1], logits, 0.0)
            stats = cols_ref[2, sl]
            for i, col in enumerate((top_l, jnp.sum(e, axis=1, keepdims=True),
                                     jnp.sum(e * logits, axis=1, keepdims=True), jnp.sum(hit, axis=1, keepdims=True))):
                stats = jnp.where(lanes == i * tiles + t, col, stats)
            cols_ref[2, sl] = stats

    finish_sum(0)
    normalize(0)
    for g in range(GROUPS):
        head(g, 0, EARLY)
        if g + 1 < GROUPS:
            finish_sum(g + 1)
        head(g, EARLY, tiles)
        if g + 1 < GROUPS:
            normalize(g + 1)

    by_row = cols_ref[2].T
    tops = by_row[:tiles]
    scale = jnp.exp(tops - jnp.max(tops, axis=0, keepdims=True))
    st_ref[me] = jnp.concatenate(
        [tops, jnp.sum(by_row[tiles:2 * tiles] * scale, axis=0, keepdims=True),
         jnp.sum(by_row[2 * tiles:3 * tiles] * scale, axis=0, keepdims=True),
         jnp.sum(by_row[3 * tiles:4 * tiles], axis=0, keepdims=True),
         jnp.zeros((st_ref.shape[1] - tiles - 3, rows), F32)], axis=0)
    send(st_ref.at[me], ids.snxt, nxt)
    send(st_ref.at[me], ids.sprv, prv)
    send(st_ref.at[me], ids.sopp, opp)
    send(st_ref.at[me], ids.sdie, die)

    sent = {}
    for g in range(GROUPS):
        for t in range(tiles):
            at = g * tiles + t
            sent["me", t, g] = list(own_sends(t, g))
            arrived(blk(prv, t, g), ids.znxt + at)
            sent["prv", t, g] = []
            sent["nxt", t, g] = []
            if t % 2 == 0:
                sent["prv", t, g].append(send(blk(prv, t, g), ids.zrel + at, nxt))
            sent["prv", t, g].append(send(blk(prv, t, g), ids.zfp + at, die))
            arrived(blk(nxt, t, g), ids.zprv + at)
            if t % 2 == 1:
                sent["nxt", t, g].append(send(blk(nxt, t, g), ids.zrel + at, prv))
            sent["nxt", t, g].append(send(blk(nxt, t, g), ids.zfn + at, die))

    arrived(st_ref.at[prv], ids.snxt)
    send(st_ref.at[prv], ids.sfp, die)
    arrived(st_ref.at[nxt], ids.sprv)
    send(st_ref.at[nxt], ids.sfn, die)
    arrived(st_ref.at[opp], ids.sopp)
    send(st_ref.at[opp], ids.sfo, die)
    for s, k in ((die, ids.sdie), (p_prv, ids.sfp), (p_nxt, ids.sfn), (p_opp, ids.sfo)):
        arrived(st_ref.at[s], k)

    dev_top = jnp.max(st_ref[:, :tiles], axis=1)
    top = jnp.max(dev_top, axis=0, keepdims=True)
    scale = jnp.exp(dev_top - top)
    sum_exp = jnp.sum(st_ref[:, tiles] * scale, axis=0, keepdims=True)
    weighted = jnp.sum(st_ref[:, tiles + 1] * scale, axis=0, keepdims=True)
    target_logit = jnp.sum(st_ref[:, tiles + 2], axis=0, keepdims=True)
    log_norm = top + jnp.log(sum_exp)
    fin_ref[0:1] = log_norm
    fin_ref[1:2] = log_norm - weighted / sum_exp
    fin_ref[2:3] = target_logit - log_norm
    pad = jnp.zeros((128 - tiles, rows), F32)

    @pl.loop(0, n)
    def _(dev):
        shift_ref[dev] = jnp.concatenate([st_ref[dev, :tiles] - log_norm, pad], axis=0).T

    done = set()

    def correct(name, dev, t):
        for g in range(GROUPS):
            for c in sent.get((name, t, g), ()):
                c.wait_send()
                done.add(id(c))
        b = dev * tiles + t
        z_ref[b] = (z_ref[b].astype(F32) + shift_ref[dev][:, t:t + 1]).astype(BF16)

    ready = []
    for t in range(tiles):
        ready += [("me", me, t), ("prv", prv, t), ("nxt", nxt, t), ("die", die, t), ("p_prv", p_prv, t), ("p_nxt", p_nxt, t)]
    landed = {"die": ids.zdie, "p_prv": ids.zfp, "p_nxt": ids.zfn, "p_opp": ids.zfo}

    def settle(name, dev, t):
        if name in landed:
            for g in range(GROUPS):
                arrived(blk(dev, t, g), landed[name] + g * tiles + t)
        correct(name, dev, t)

    steps = GROUPS * tiles
    taken = 0
    for g in range(GROUPS):
        for t in range(tiles):
            at = g * tiles + t
            upto = (at * len(ready)) // (steps - 1)
            for item in ready[taken:upto]:
                settle(*item)
            taken = max(taken, upto)
            arrived(blk(opp, t, g), ids.zrel + at)
            sent["opp", t, g] = [send(blk(opp, t, g), ids.zfo + at, die)]
            if g == GROUPS - 1 and t > 0:
                settle("opp", opp, t - 1)
                settle("p_opp", p_opp, t - 1)
    settle("opp", opp, tiles - 1)
    settle("p_opp", p_opp, tiles - 1)
    for c in copies:
        if id(c) not in done:
            c.wait_send()


def finish_kernel(z_ref, fin_ref, norm_ref, ent_ref, logp_ref, out_hbm, sem):
    blocks, rows, width = z_ref.shape

    def put(b):
        return pltpu.make_async_copy(
            z_ref.at[b], out_hbm.at[:, pl.ds(pl.multiple_of(b * width, width), width)], sem.at[b])

    @pl.loop(0, blocks)
    def _(b):
        put(b).start()

    norm_ref[...] = fin_ref[0:1]
    ent_ref[...] = fin_ref[1:2]
    logp_ref[...] = fin_ref[2:3]

    @pl.loop(0, blocks)
    def _(b):
        put(b).wait()


def solution(mesh):
    n = mesh.shape["tp"]

    def device_step(hidden, w_gate, w_up, w_down, norm_gain, w_vocab, temperature, target):
        rows, dim = hidden.shape
        f_loc = w_gate.shape[1]
        v_loc = w_vocab.shape[1]
        own_w = dim // n
        tiles = v_loc // TILE
        n_ids = Ids(n // 2, tiles).count
        any_spec = pl.BlockSpec(memory_space=pl.ANY)
        vmem = pl.BlockSpec(memory_space=pltpu.VMEM)
        z, fin = pl.pallas_call(
            functools.partial(main_kernel, n),
            out_shape=(pltpu.VMEM((n * tiles, rows, TILE), BF16), pltpu.VMEM((8, rows), F32)),
            in_specs=[any_spec] * 8,
            out_specs=(vmem, vmem),
            scratch_shapes=[
                pltpu.VMEM((v_loc // SLAB, dim, SLAB), BF16),
                pltpu.VMEM((DOWN_SLOTS, f_loc, own_w), BF16),
                pltpu.VMEM((rows, dim), BF16),
                pltpu.VMEM((rows, dim), BF16),
                pltpu.VMEM((rows, f_loc), BF16),
                pltpu.VMEM((1, dim), F32),
                pltpu.VMEM((1, rows), F32),
                pltpu.VMEM((1, rows), jnp.int32),
                pltpu.VMEM((4, rows, own_w), BF16),
                pltpu.VMEM((4, rows, own_w), BF16),
                pltpu.VMEM((rows, own_w), BF16),
                pltpu.VMEM((rows, own_w), BF16),
                pltpu.VMEM((2, rows, own_w), BF16),
                pltpu.VMEM((2, rows, own_w), BF16),
                pltpu.VMEM((3, rows, own_w), F32),
                pltpu.VMEM((n, rows, own_w), BF16),
                pltpu.VMEM((3, rows, 128), F32),
                pltpu.VMEM((n, 16, rows), F32),
                pltpu.VMEM((n, rows, 128), F32),
                pltpu.SemaphoreType.DMA((n_ids,)),
                pltpu.SemaphoreType.DMA((n_ids,)),
                pltpu.SemaphoreType.DMA((5, v_loc // SLAB)),
                pltpu.SemaphoreType.DMA((n,)),
                pltpu.SemaphoreType.DMA((4,)),
            ],
            compiler_params=pltpu.CompilerParams(
                collective_id=0, has_side_effects=True, vmem_limit_bytes=55 * 1024 * 1024),
            name="decode_tail",
        )(hidden, w_gate, w_up, w_down, norm_gain.reshape(1, dim), w_vocab, temperature.reshape(1, rows),
          target.reshape(1, rows))
        row = jax.ShapeDtypeStruct((1, rows), F32)
        log_norm, entropy, target_logp, log_probs = pl.pallas_call(
            finish_kernel,
            out_shape=(row, row, row, jax.ShapeDtypeStruct((rows, n * v_loc), BF16)),
            in_specs=[vmem, vmem],
            out_specs=(vmem, vmem, vmem, any_spec),
            scratch_shapes=[pltpu.SemaphoreType.DMA((n * tiles,))],
            compiler_params=pltpu.CompilerParams(vmem_limit_bytes=4 * 1024 * 1024),
            name="write_log_probs",
        )(z, fin)
        return log_norm.reshape(rows), entropy.reshape(rows), target_logp.reshape(rows), log_probs

    return jax.shard_map(
        device_step,
        mesh=mesh,
        in_specs=(P("dp", None), P(None, "tp"), P(None, "tp"), P("tp", None), P(None),
                  P(None, "tp"), P("dp"), P("dp")),
        out_specs=(P("dp"), P("dp"), P("dp"), P("dp", None)),
        check_vma=False,
    )
```

```python
import functools

import jax
import jax.numpy as jnp
from jax import lax
from jax.experimental import pallas as pl
from jax.experimental.pallas import tpu as pltpu
from jax.sharding import PartitionSpec as P

NORM_EPS = 1e-6
MESH = pl.DeviceIdType.MESH
F32 = jnp.float32
BF16 = jnp.bfloat16

SLAB = 256
AHEAD = 3
DOWN_AHEAD = 3
DOWN_SLOTS = 4
SPLIT = (1, 3)
GROUPS = len(SPLIT)
TILE = 512
EARLY = 3


class Ids:
    def __init__(self, chips, tiles):
        self.count = 0
        g = GROUPS
        self.part = self.take(chips)
        self.rs = self.take(3 * g)
        self.ynxt, self.yprv, self.yopp, self.ydie, self.fprv, self.fnxt, self.fopp = (self.take(g) for _ in range(7))
        self.znxt, self.zprv, self.zdie, self.zrel, self.zfp, self.zfn, self.zfo = (
            self.take(g * tiles) for _ in range(7))
        self.snxt, self.sprv, self.sopp, self.sdie, self.sfp, self.sfn, self.sfo = (self.take(1) for _ in range(7))

    def take(self, k):
        first = self.count
        self.count += k
        return first


def main_kernel(n, h_hbm, wg_hbm, wu_hbm, wd_hbm, gain_hbm, wv_hbm, temp_hbm, targ_hbm,
                z_ref, fin_ref,
                wbuf, dbuf, h_ref, a_ref, gu_ref, gain_ref, temp_ref, targ_ref,
                psend, prcv, rsend, rrcv, own_ref, ygat, cols_ref, st_ref, shift_ref, raw_ref,
                ss, rs, wsem, dsem, msem):
    chips = n // 2
    rows, dim = h_ref.shape
    unit = rows // sum(SPLIT)
    sizes = [unit * k for k in SPLIT]
    starts = [unit * sum(SPLIT[:g]) for g in range(GROUPS)]
    f_loc = a_ref.shape[1]
    nf = f_loc // SLAB
    own_w = dim // n
    tiles = z_ref.shape[0] // n
    per_tile = TILE // SLAB
    ids = Ids(chips, tiles)

    me = lax.axis_index("tp")
    chip, core = me // 2, me % 2
    other = 1 - core
    c_nxt, c_prv, c_opp = (chip + 1) % chips, (chip + chips - 1) % chips, (chip + 2) % chips
    nxt, prv, opp = c_nxt * 2 + core, c_prv * 2 + core, c_opp * 2 + core
    die = chip * 2 + other
    p_prv, p_nxt, p_opp = c_prv * 2 + other, c_nxt * 2 + other, c_opp * 2 + other

    def remote(src, dst, k, dev):
        return pltpu.make_async_remote_copy(src_ref=src, dst_ref=dst, send_sem=ss.at[k], recv_sem=rs.at[k],
                                            device_id={"tp": dev}, device_id_type=MESH)

    copies = []

    def send(ref, k, dev):
        c = remote(ref, ref, k, dev)
        c.start()
        copies.append(c)
        return c

    def arrived(ref, k):
        remote(ref, ref, k, die).wait_recv()

    def g_rows(g):
        return pl.ds(starts[g], sizes[g])

    def g_slice(g):
        return slice(starts[g], starts[g] + sizes[g])

    small = [pltpu.make_async_copy(h_hbm, h_ref, msem.at[0]),
             pltpu.make_async_copy(gain_hbm, gain_ref, msem.at[1]),
             pltpu.make_async_copy(temp_hbm, temp_ref, msem.at[2]),
             pltpu.make_async_copy(targ_hbm, targ_ref, msem.at[3])]

    def gate_up(j):
        col = pl.ds(pl.multiple_of(j * SLAB, SLAB), SLAB)
        return (pltpu.make_async_copy(wg_hbm.at[:, col], wbuf.at[2 * j], wsem.at[0, j]),
                pltpu.make_async_copy(wu_hbm.at[:, col], wbuf.at[2 * j + 1], wsem.at[1, j]))

    def start_gate_up(j):
        for c in gate_up(j):
            c.start()

    def vocab(s):
        col = pl.ds(pl.multiple_of(s * SLAB, SLAB), SLAB)
        return pltpu.make_async_copy(wv_hbm.at[:, col], wbuf.at[s], wsem.at[2, s])

    def down(k, dev):
        col = pl.ds(pl.multiple_of(dev * own_w, own_w), own_w)
        return pltpu.make_async_copy(wd_hbm.at[:, col], dbuf.at[k % DOWN_SLOTS], dsem.at[k])

    plan = ((c_opp, 0, True), (c_nxt, 1, True), (c_opp, 0, False), (c_prv, 2, True),
            (c_nxt, 1, False), (chip, 3, True), (c_prv, 2, False), (chip, 3, False))
    order = [c * 2 + (other if away else core) for c, _, away in plan]

    small[0].start()
    for j in range(AHEAD):
        start_gate_up(j)
    for c in small[1:]:
        c.start()

    barrier = pltpu.get_barrier_semaphore()
    for r in range(1, n):
        pl.semaphore_signal(barrier, inc=1, device_id={"tp": (me + r) % n}, device_id_type=MESH)

    small[0].wait()
    gu_ref[...] = jnp.zeros_like(gu_ref)

    def activate(j):
        act = jax.nn.silu(gu_ref[0]) * gu_ref[1]
        a_ref[:, pl.ds(pl.multiple_of(j * SLAB, SLAB), SLAB)] = act.astype(BF16)

    @pl.loop(0, nf)
    def _(j):
        for c in gate_up(j):
            c.wait()

        @pl.when(j + AHEAD < nf)
        def _():
            start_gate_up(j + AHEAD)

        for k in range(DOWN_AHEAD):
            @pl.when(j == nf - AHEAD + min(k, AHEAD - 1))
            def _():
                down(k, order[k]).start()

        activate(jnp.maximum(j - 1, 0))
        gate = jnp.dot(h_ref[...], wbuf[2 * j], preferred_element_type=F32)
        up = jnp.dot(h_ref[...], wbuf[2 * j + 1], preferred_element_type=F32)
        gu_ref[0] = gate
        gu_ref[1] = up

    activate(nf - 1)

    n_down = len(plan)
    owners = (opp, nxt, prv)

    def reduce_send(q, g):
        c = remote(rsend.at[q, g_rows(g)], rrcv.at[q, g_rows(g)], ids.rs + q * GROUPS + g, owners[q])
        c.start()
        copies.append(c)

    for k, (_, q, away) in enumerate(plan):
        if k + DOWN_AHEAD < n_down:
            down(k + DOWN_AHEAD, order[k + DOWN_AHEAD]).start()
        else:
            per = (tiles * per_tile) // DOWN_AHEAD
            first = (k + DOWN_AHEAD - n_down) * per
            last = tiles * per_tile if k == n_down - 1 else first + per
            for s in range(first, last):
                vocab(s).start()
        down(k, order[k]).wait()
        part = jnp.dot(a_ref[...], dbuf[k % DOWN_SLOTS], preferred_element_type=F32)
        to_die = remote(psend.at[q], prcv.at[q], ids.part + q, die)
        if k == 0:
            pl.semaphore_wait(barrier, n - 1)
        if away:
            psend[q] = part.astype(BF16)
            to_die.start()
            copies.append(to_die)
            continue
        to_die.wait_recv()
        total = part + prcv[q].astype(F32)
        if q < 3:
            rsend[q] = total.astype(BF16)
            reduce_send(q, 0)
        else:
            own_ref[...] = total

    for c in small[1:]:
        c.wait()
    row_ids = lax.broadcasted_iota(jnp.int32, (rows, rows), 0)
    lane_ids = lax.broadcasted_iota(jnp.int32, (rows, rows), 1)
    eye = row_ids == lane_ids
    inv_temp = 1.0 / jnp.sum(jnp.where(eye, temp_ref[...], 0.0), axis=1, keepdims=True)
    targ = jnp.sum(jnp.where(eye, targ_ref[...].astype(F32), 0.0), axis=1, keepdims=True)
    cols_ref[0] = jnp.broadcast_to(inv_temp, (rows, 128))
    cols_ref[1] = jnp.broadcast_to(targ, (rows, 128))
    cols_ref[2] = jnp.zeros((rows, 128), F32)

    def sum_and_send(g):
        sl = g_slice(g)
        for q in range(3):
            arrived(rrcv.at[q, g_rows(g)], ids.rs + q * GROUPS + g)
        y = own_ref[sl] + rrcv[0, sl].astype(F32) + rrcv[1, sl].astype(F32) + rrcv[2, sl].astype(F32)
        ygat[me, sl] = y.astype(BF16)
        own = ygat.at[me, g_rows(g)]
        send(own, ids.yopp + g, opp)
        send(own, ids.ynxt + g, nxt)
        send(own, ids.yprv + g, prv)
        send(own, ids.ydie + g, die)

    def residual(s, g):
        col = pl.ds(pl.multiple_of(s * own_w, own_w), own_w)
        return col, h_ref[g_rows(g), col].astype(F32) + ygat[s, g_slice(g)].astype(F32)

    def squares(s, g):
        _, r = residual(s, g)
        return jnp.sum(r * r, axis=1, keepdims=True)

    def finish_sum(g):
        for s, k, f in ((prv, ids.ynxt, ids.fprv), (nxt, ids.yprv, ids.fnxt), (opp, ids.yopp, ids.fopp)):
            arrived(ygat.at[s, g_rows(g)], k + g)
            send(ygat.at[s, g_rows(g)], f + g, die)

    def normalize(g):
        total_sq = squares(me, g) + squares(prv, g) + squares(nxt, g) + squares(opp, g)
        for s, k in ((die, ids.ydie), (p_prv, ids.fprv), (p_nxt, ids.fnxt), (p_opp, ids.fopp)):
            arrived(ygat.at[s, g_rows(g)], k + g)
            total_sq += squares(s, g)
        inv_rms = lax.rsqrt(total_sq * (1.0 / dim) + NORM_EPS)

        @pl.loop(0, n)
        def _(s):
            col, r = residual(s, g)
            h_ref[g_rows(g), col] = (gain_ref[:, col] * r * inv_rms).astype(BF16)


    def blk(dev, t, g):
        return raw_ref.at[dev * tiles + t, g_rows(g)]

    def own_sends(t, g):
        b = blk(me, t, g)
        at = g * tiles + t
        return (remote(b, b, ids.znxt + at, nxt), remote(b, b, ids.zprv + at, prv), remote(b, b, ids.zdie + at, die))

    def head(g, t0, t1):
        sl = g_slice(g)
        lanes = lax.broadcasted_iota(jnp.int32, (sizes[g], 128), 1)

        @pl.loop(t0, t1)
        def _(t):
            if g == 0:
                for i in range(per_tile):
                    vocab(t * per_tile + i).wait()
            pieces = [jnp.dot(h_ref[sl], wbuf[t * per_tile + i], preferred_element_type=F32) for i in range(per_tile)]
            logits = jnp.concatenate(pieces, axis=1) * cols_ref[0, sl][:, :1]
            top_l = jnp.max(logits, axis=1, keepdims=True)
            low = logits - top_l
            raw_ref[me * tiles + t, sl] = low.astype(BF16)
            for c in own_sends(t, g):
                c.start()
            e = jnp.exp(low)
            col_ids = lax.broadcasted_iota(jnp.int32, (sizes[g], TILE), 1) + (me * tiles + t) * TILE
            hit = jnp.where(col_ids.astype(F32) == cols_ref[1, sl][:, :1], logits, 0.0)
            stats = cols_ref[2, sl]
            for i, col in enumerate((top_l, jnp.sum(e, axis=1, keepdims=True),
                                     jnp.sum(e * logits, axis=1, keepdims=True), jnp.sum(hit, axis=1, keepdims=True))):
                stats = jnp.where(lanes == i * tiles + t, col, stats)
            cols_ref[2, sl] = stats

    sum_and_send(0)
    for g in range(1, GROUPS):
        for q in range(3):
            reduce_send(q, g)
    finish_sum(0)
    normalize(0)
    for g in range(GROUPS):
        head(g, 0, EARLY)
        if g + 1 < GROUPS:
            sum_and_send(g + 1)
        head(g, EARLY, tiles)
        if g + 1 < GROUPS:
            finish_sum(g + 1)
            normalize(g + 1)

    by_row = cols_ref[2].T
    tops = by_row[:tiles]
    scale = jnp.exp(tops - jnp.max(tops, axis=0, keepdims=True))
    st_ref[me] = jnp.concatenate(
        [tops, jnp.sum(by_row[tiles:2 * tiles] * scale, axis=0, keepdims=True),
         jnp.sum(by_row[2 * tiles:3 * tiles] * scale, axis=0, keepdims=True),
         jnp.sum(by_row[3 * tiles:4 * tiles], axis=0, keepdims=True),
         jnp.zeros((st_ref.shape[1] - tiles - 3, rows), F32)], axis=0)
    send(st_ref.at[me], ids.snxt, nxt)
    send(st_ref.at[me], ids.sprv, prv)
    send(st_ref.at[me], ids.sopp, opp)
    send(st_ref.at[me], ids.sdie, die)

    for g in range(GROUPS):
        for t in range(tiles):
            at = g * tiles + t
            copies += own_sends(t, g)
            arrived(blk(prv, t, g), ids.znxt + at)
            if t % 2 == 0:
                send(blk(prv, t, g), ids.zrel + at, nxt)
            send(blk(prv, t, g), ids.zfp + at, die)
            arrived(blk(nxt, t, g), ids.zprv + at)
            if t % 2 == 1:
                send(blk(nxt, t, g), ids.zrel + at, prv)
            send(blk(nxt, t, g), ids.zfn + at, die)

    arrived(st_ref.at[prv], ids.snxt)
    send(st_ref.at[prv], ids.sfp, die)
    arrived(st_ref.at[nxt], ids.sprv)
    send(st_ref.at[nxt], ids.sfn, die)
    arrived(st_ref.at[opp], ids.sopp)
    send(st_ref.at[opp], ids.sfo, die)
    for s, k in ((die, ids.sdie), (p_prv, ids.sfp), (p_nxt, ids.sfn), (p_opp, ids.sfo)):
        arrived(st_ref.at[s], k)

    dev_top = jnp.max(st_ref[:, :tiles], axis=1)
    top = jnp.max(dev_top, axis=0, keepdims=True)
    scale = jnp.exp(dev_top - top)
    sum_exp = jnp.sum(st_ref[:, tiles] * scale, axis=0, keepdims=True)
    weighted = jnp.sum(st_ref[:, tiles + 1] * scale, axis=0, keepdims=True)
    target_logit = jnp.sum(st_ref[:, tiles + 2], axis=0, keepdims=True)
    log_norm = top + jnp.log(sum_exp)
    fin_ref[0:1] = log_norm
    fin_ref[1:2] = log_norm - weighted / sum_exp
    fin_ref[2:3] = target_logit - log_norm
    pad = jnp.zeros((128 - tiles, rows), F32)

    for dev in range(n):
        shift_ref[dev] = jnp.concatenate([st_ref[dev, :tiles] - log_norm, pad], axis=0).T

    ready = []
    for t in range(tiles):
        ready += [("me", me, t), ("prv", prv, t), ("nxt", nxt, t), ("die", die, t), ("p_prv", p_prv, t), ("p_nxt", p_nxt, t)]
    landed = {"die": ids.zdie, "p_prv": ids.zfp, "p_nxt": ids.zfn, "p_opp": ids.zfo}

    def settle(items):
        for name, dev, t in items:
            if name in landed:
                for g in range(GROUPS):
                    arrived(blk(dev, t, g), landed[name] + g * tiles + t)
        for _, dev, t in items:
            b = dev * tiles + t
            z_ref[b] = (raw_ref[b].astype(F32) + shift_ref[dev][:, t:t + 1]).astype(BF16)

    steps = GROUPS * tiles
    taken = 0
    for g in range(GROUPS):
        for t in range(tiles):
            at = g * tiles + t
            upto = max(taken, (at * len(ready)) // (steps - 1))
            batch = ready[taken:upto]
            taken = upto
            if g == GROUPS - 1 and t > 1:
                batch += [("opp", opp, t - 2), ("p_opp", p_opp, t - 2)]
            settle(batch)
            arrived(blk(opp, t, g), ids.zrel + at)
            send(blk(opp, t, g), ids.zfo + at, die)
    settle([("opp", opp, tiles - 2), ("opp", opp, tiles - 1), ("p_opp", p_opp, tiles - 2)])
    settle([("p_opp", p_opp, tiles - 1)])
    for c in copies:
        c.wait_send()


def finish_kernel(z_ref, fin_ref, norm_hbm, ent_hbm, logp_hbm, out_hbm, sem):
    blocks, rows, width = z_ref.shape

    def put(b):
        return pltpu.make_async_copy(
            z_ref.at[b], out_hbm.at[:, pl.ds(pl.multiple_of(b * width, width), width)], sem.at[b])

    @pl.loop(0, blocks)
    def _(b):
        put(b).start()

    small = [pltpu.make_async_copy(fin_ref.at[pl.ds(i, 1)], ref, sem.at[blocks + i])
             for i, ref in enumerate((norm_hbm, ent_hbm, logp_hbm))]
    for c in small:
        c.start()

    @pl.loop(0, blocks)
    def _(b):
        put(b).wait()

    for c in small:
        c.wait()


def solution(mesh):
    n = mesh.shape["tp"]

    def device_step(hidden, w_gate, w_up, w_down, norm_gain, w_vocab, temperature, target):
        rows, dim = hidden.shape
        f_loc = w_gate.shape[1]
        v_loc = w_vocab.shape[1]
        own_w = dim // n
        tiles = v_loc // TILE
        n_ids = Ids(n // 2, tiles).count
        any_spec = pl.BlockSpec(memory_space=pl.ANY)
        vmem = pl.BlockSpec(memory_space=pltpu.VMEM)
        z, fin = pl.pallas_call(
            functools.partial(main_kernel, n),
            out_shape=(pltpu.VMEM((n * tiles, rows, TILE), BF16), pltpu.VMEM((8, rows), F32)),
            in_specs=[any_spec] * 8,
            out_specs=(vmem, vmem),
            scratch_shapes=[
                pltpu.VMEM((v_loc // SLAB, dim, SLAB), BF16),
                pltpu.VMEM((DOWN_SLOTS, f_loc, own_w), BF16),
                pltpu.VMEM((rows, dim), BF16),
                pltpu.VMEM((rows, f_loc), BF16),
                pltpu.VMEM((2, rows, SLAB), F32),
                pltpu.VMEM((1, dim), F32),
                pltpu.VMEM((1, rows), F32),
                pltpu.VMEM((1, rows), jnp.int32),
                pltpu.VMEM((4, rows, own_w), BF16),
                pltpu.VMEM((4, rows, own_w), BF16),
                pltpu.VMEM((3, rows, own_w), BF16),
                pltpu.VMEM((3, rows, own_w), BF16),
                pltpu.VMEM((rows, own_w), F32),
                pltpu.VMEM((n, rows, own_w), BF16),
                pltpu.VMEM((3, rows, 128), F32),
                pltpu.VMEM((n, 16, rows), F32),
                pltpu.VMEM((n, rows, 128), F32),
                pltpu.VMEM((n * tiles, rows, TILE), BF16),
                pltpu.SemaphoreType.DMA((n_ids,)),
                pltpu.SemaphoreType.DMA((n_ids,)),
                pltpu.SemaphoreType.DMA((3, v_loc // SLAB)),
                pltpu.SemaphoreType.DMA((n,)),
                pltpu.SemaphoreType.DMA((4,)),
            ],
            compiler_params=pltpu.CompilerParams(
                collective_id=0, has_side_effects=True, vmem_limit_bytes=57100 * 1024),
            name="decode_tail",
        )(hidden, w_gate, w_up, w_down, norm_gain.reshape(1, dim), w_vocab, temperature.reshape(1, rows),
          target.reshape(1, rows))
        row = jax.ShapeDtypeStruct((1, rows), F32)
        log_norm, entropy, target_logp, log_probs = pl.pallas_call(
            finish_kernel,
            out_shape=(row, row, row, jax.ShapeDtypeStruct((rows, n * v_loc), BF16)),
            in_specs=[vmem, vmem],
            out_specs=(any_spec,) * 4,
            scratch_shapes=[pltpu.SemaphoreType.DMA((n * tiles + 3,))],
            compiler_params=pltpu.CompilerParams(vmem_limit_bytes=4 * 1024 * 1024),
            name="write_log_probs",
        )(z, fin)
        return log_norm.reshape(rows), entropy.reshape(rows), target_logp.reshape(rows), log_probs

    return jax.shard_map(
        device_step,
        mesh=mesh,
        in_specs=(P("dp", None), P(None, "tp"), P(None, "tp"), P("tp", None), P(None),
                  P(None, "tp"), P("dp"), P("dp")),
        out_specs=(P("dp"), P("dp"), P("dp"), P("dp", None)),
        check_vma=False,
    )
```

```python
import functools

import jax
import jax.numpy as jnp
from jax import lax
from jax.experimental import pallas as pl
from jax.experimental.pallas import tpu as pltpu
from jax.sharding import PartitionSpec as P

NORM_EPS = 1e-6
MESH = pl.DeviceIdType.MESH
F32 = jnp.float32
BF16 = jnp.bfloat16

SLAB = 256
AHEAD = 3
DOWN_AHEAD = 3
DOWN_SLOTS = 4
SPLIT = (3, 5)
GROUPS = len(SPLIT)
RELAYED = 6
TILE = 512
EARLY = 6


class Ids:
    def __init__(self, chips, tiles):
        self.count = 0
        g = GROUPS
        self.part = self.take(chips)
        self.rs = self.take(3 * g)
        self.ynxt, self.yprv, self.yopp, self.ydie, self.fprv, self.fnxt, self.fopp = (self.take(g) for _ in range(7))
        self.znxt, self.zprv, self.zdie, self.zrel, self.zfp, self.zfn, self.zfo = (
            self.take(g * tiles) for _ in range(7))
        self.snxt, self.sprv, self.sopp, self.sdie, self.sfp, self.sfn, self.sfo = (self.take(1) for _ in range(7))

    def take(self, k):
        first = self.count
        self.count += k
        return first


def main_kernel(n, h_hbm, wg_hbm, wu_hbm, wd_hbm, gain_hbm, wv_hbm, temp_hbm, targ_hbm,
                z_ref, fin_ref,
                wbuf, dbuf, h_ref, a_ref, gu_ref, gain_ref, temp_ref, targ_ref,
                psend, prcv, rsend, rrcv, own_ref, ygat, cols_ref, st_ref, shift_ref, raw_ref,
                ss, rs, wsem, dsem, msem):
    chips = n // 2
    rows, dim = h_ref.shape
    unit = rows // sum(SPLIT)
    sizes = [unit * k for k in SPLIT]
    starts = [unit * sum(SPLIT[:g]) for g in range(GROUPS)]
    f_loc = a_ref.shape[1]
    nf = f_loc // SLAB
    own_w = dim // n
    tiles = z_ref.shape[0] // n
    per_tile = TILE // SLAB
    ids = Ids(chips, tiles)

    me = lax.axis_index("tp")
    chip, core = me // 2, me % 2
    other = 1 - core
    c_nxt, c_prv, c_opp = (chip + 1) % chips, (chip + chips - 1) % chips, (chip + 2) % chips
    nxt, prv, opp = c_nxt * 2 + core, c_prv * 2 + core, c_opp * 2 + core
    die = chip * 2 + other
    p_prv, p_nxt, p_opp = c_prv * 2 + other, c_nxt * 2 + other, c_opp * 2 + other

    def remote(src, dst, k, dev):
        return pltpu.make_async_remote_copy(src_ref=src, dst_ref=dst, send_sem=ss.at[k], recv_sem=rs.at[k],
                                            device_id={"tp": dev}, device_id_type=MESH)

    copies = []

    def send(ref, k, dev):
        c = remote(ref, ref, k, dev)
        c.start()
        copies.append(c)
        return c

    def arrived(ref, k):
        remote(ref, ref, k, die).wait_recv()

    def g_rows(g):
        return pl.ds(starts[g], sizes[g])

    def g_slice(g):
        return slice(starts[g], starts[g] + sizes[g])

    small = [pltpu.make_async_copy(h_hbm, h_ref, msem.at[0]),
             pltpu.make_async_copy(gain_hbm, gain_ref, msem.at[1]),
             pltpu.make_async_copy(temp_hbm, temp_ref, msem.at[2]),
             pltpu.make_async_copy(targ_hbm, targ_ref, msem.at[3])]

    def gate_up(j):
        col = pl.ds(pl.multiple_of(j * SLAB, SLAB), SLAB)
        return (pltpu.make_async_copy(wg_hbm.at[:, col], wbuf.at[2 * j], wsem.at[0, j]),
                pltpu.make_async_copy(wu_hbm.at[:, col], wbuf.at[2 * j + 1], wsem.at[1, j]))

    def last_pair(part):
        rws = pl.ds(part * (dim // 2), dim // 2)
        col = pl.ds((nf - 1) * SLAB, SLAB)
        return (pltpu.make_async_copy(wg_hbm.at[rws, col], wbuf.at[2 * nf - 2, rws], wsem.at[0, nf - 1 + part]),
                pltpu.make_async_copy(wu_hbm.at[rws, col], wbuf.at[2 * nf - 1, rws], wsem.at[1, nf - 1 + part]))

    def start_gate_up(j):
        @pl.when(j < nf - 1)
        def _():
            for c in gate_up(j):
                c.start()

        @pl.when(j == nf - 1)
        def _():
            for c in last_pair(0) + last_pair(1):
                c.start()

    def vocab(s):
        col = pl.ds(pl.multiple_of(s * SLAB, SLAB), SLAB)
        return pltpu.make_async_copy(wv_hbm.at[:, col], wbuf.at[s], wsem.at[2, s])

    def down(k, dev):
        col = pl.ds(pl.multiple_of(dev * own_w, own_w), own_w)
        return pltpu.make_async_copy(wd_hbm.at[:, col], dbuf.at[k % DOWN_SLOTS], dsem.at[k])

    plan = ((c_opp, 0, True), (c_nxt, 1, True), (c_prv, 2, True), (c_opp, 0, False),
            (c_nxt, 1, False), (c_prv, 2, False), (chip, 3, True), (chip, 3, False))
    order = [c * 2 + (other if away else core) for c, _, away in plan]

    small[0].start()
    for j in range(AHEAD):
        start_gate_up(j)
    for c in small[1:]:
        c.start()

    barrier = pltpu.get_barrier_semaphore()
    for r in range(1, n):
        pl.semaphore_signal(barrier, inc=1, device_id={"tp": (me + r) % n}, device_id_type=MESH)

    small[0].wait()
    gu_ref[...] = jnp.zeros_like(gu_ref)

    def activate(j):
        act = jax.nn.silu(gu_ref[0]) * gu_ref[1]
        a_ref[:, pl.ds(pl.multiple_of(j * SLAB, SLAB), SLAB)] = act.astype(BF16)

    @pl.loop(0, nf - 1)
    def _(j):
        for c in gate_up(j):
            c.wait()

        @pl.when(j + AHEAD < nf)
        def _():
            start_gate_up(j + AHEAD)

        for k in range(DOWN_AHEAD):
            @pl.when(j == nf - AHEAD + min(k, AHEAD - 2))
            def _():
                down(k, order[k]).start()

        activate(jnp.maximum(j - 1, 0))
        gate = jnp.dot(h_ref[...], wbuf[2 * j], preferred_element_type=F32)
        up = jnp.dot(h_ref[...], wbuf[2 * j + 1], preferred_element_type=F32)
        gu_ref[0] = gate
        gu_ref[1] = up

    for c in last_pair(0):
        c.wait()
    kh = dim // 2
    activate(nf - 2)
    gu_ref[0] = jnp.dot(h_ref[:, :kh], wbuf[2 * nf - 2, :kh], preferred_element_type=F32)
    gu_ref[1] = jnp.dot(h_ref[:, :kh], wbuf[2 * nf - 1, :kh], preferred_element_type=F32)
    for c in last_pair(1):
        c.wait()
    gu_ref[0] += jnp.dot(h_ref[:, kh:], wbuf[2 * nf - 2, kh:], preferred_element_type=F32)
    gu_ref[1] += jnp.dot(h_ref[:, kh:], wbuf[2 * nf - 1, kh:], preferred_element_type=F32)
    activate(nf - 1)

    n_down = len(plan)
    owners = (opp, nxt, prv)

    def reduce_send(q, g):
        c = remote(rsend.at[q, g_rows(g)], rrcv.at[q, g_rows(g)], ids.rs + q * GROUPS + g, owners[q])
        c.start()
        copies.append(c)

    for k, (_, q, away) in enumerate(plan):
        if k + DOWN_AHEAD < n_down:
            down(k + DOWN_AHEAD, order[k + DOWN_AHEAD]).start()
        else:
            per = (tiles * per_tile) // DOWN_AHEAD
            first = (k + DOWN_AHEAD - n_down) * per
            last = tiles * per_tile if k == n_down - 1 else first + per
            for s in range(first, last):
                vocab(s).start()
        down(k, order[k]).wait()
        part = jnp.dot(a_ref[...], dbuf[k % DOWN_SLOTS], preferred_element_type=F32)
        to_die = remote(psend.at[q], prcv.at[q], ids.part + q, die)
        if k == 0:
            pl.semaphore_wait(barrier, n - 1)
        if away:
            psend[q] = part.astype(BF16)
            to_die.start()
            copies.append(to_die)
            continue
        to_die.wait_recv()
        total = part + prcv[q].astype(F32)
        if q < 3:
            rsend[q] = total.astype(BF16)
            reduce_send(q, 0)
            if q == 2:
                for g in range(1, GROUPS):
                    for r in range(3):
                        reduce_send(r, g)
        else:
            own_ref[...] = total

    for c in small[1:]:
        c.wait()
    row_ids = lax.broadcasted_iota(jnp.int32, (rows, rows), 0)
    lane_ids = lax.broadcasted_iota(jnp.int32, (rows, rows), 1)
    eye = row_ids == lane_ids
    inv_temp = 1.0 / jnp.sum(jnp.where(eye, temp_ref[...], 0.0), axis=1, keepdims=True)
    targ = jnp.sum(jnp.where(eye, targ_ref[...].astype(F32), 0.0), axis=1, keepdims=True)
    cols_ref[0] = jnp.broadcast_to(inv_temp, (rows, 128))
    cols_ref[1] = jnp.broadcast_to(targ, (rows, 128))
    cols_ref[2] = jnp.zeros((rows, 128), F32)

    def sum_and_send(g):
        sl = g_slice(g)
        for q in range(3):
            arrived(rrcv.at[q, g_rows(g)], ids.rs + q * GROUPS + g)
        y = own_ref[sl] + rrcv[0, sl].astype(F32) + rrcv[1, sl].astype(F32) + rrcv[2, sl].astype(F32)
        ygat[me, sl] = y.astype(BF16)
        own = ygat.at[me, g_rows(g)]
        send(own, ids.yopp + g, opp)
        send(own, ids.ynxt + g, nxt)
        send(own, ids.yprv + g, prv)
        send(own, ids.ydie + g, die)

    def residual(s, g):
        col = pl.ds(pl.multiple_of(s * own_w, own_w), own_w)
        return col, h_ref[g_rows(g), col].astype(F32) + ygat[s, g_slice(g)].astype(F32)

    def squares(s, g):
        _, r = residual(s, g)
        return jnp.sum(r * r, axis=1, keepdims=True)

    def finish_sum(g):
        for s, k, f in ((prv, ids.ynxt, ids.fprv), (nxt, ids.yprv, ids.fnxt), (opp, ids.yopp, ids.fopp)):
            arrived(ygat.at[s, g_rows(g)], k + g)
            send(ygat.at[s, g_rows(g)], f + g, die)

    def normalize(g):
        total_sq = squares(me, g) + squares(prv, g) + squares(nxt, g) + squares(opp, g)
        for s, k in ((die, ids.ydie), (p_prv, ids.fprv), (p_nxt, ids.fnxt), (p_opp, ids.fopp)):
            arrived(ygat.at[s, g_rows(g)], k + g)
            total_sq += squares(s, g)
        inv_rms = lax.rsqrt(total_sq * (1.0 / dim) + NORM_EPS)

        @pl.loop(0, n)
        def _(s):
            col, r = residual(s, g)
            h_ref[g_rows(g), col] = (gain_ref[:, col] * r * inv_rms).astype(BF16)


    def blk(dev, t, g):
        return raw_ref.at[dev * tiles + t, g_rows(g)]

    def own_sends(t, g):
        b = blk(me, t, g)
        at = g * tiles + t
        return (remote(b, b, ids.znxt + at, nxt), remote(b, b, ids.zprv + at, prv), remote(b, b, ids.zdie + at, die))

    def head(g, t0, t1):
        sl = g_slice(g)
        lanes = lax.broadcasted_iota(jnp.int32, (sizes[g], 128), 1)

        @pl.loop(t0, t1)
        def _(t):
            if g == 0:
                for i in range(per_tile):
                    vocab(t * per_tile + i).wait()
            pieces = [jnp.dot(h_ref[sl], wbuf[t * per_tile + i], preferred_element_type=F32) for i in range(per_tile)]
            logits = jnp.concatenate(pieces, axis=1) * cols_ref[0, sl][:, :1]
            top_l = jnp.max(logits, axis=1, keepdims=True)
            low = logits - top_l
            raw_ref[me * tiles + t, sl] = low.astype(BF16)
            for c in own_sends(t, g):
                c.start()
            e = jnp.exp(low)
            col_ids = lax.broadcasted_iota(jnp.int32, (sizes[g], TILE), 1) + (me * tiles + t) * TILE
            hit = jnp.where(col_ids.astype(F32) == cols_ref[1, sl][:, :1], logits, 0.0)
            stats = cols_ref[2, sl]
            for i, col in enumerate((top_l, jnp.sum(e, axis=1, keepdims=True),
                                     jnp.sum(e * logits, axis=1, keepdims=True), jnp.sum(hit, axis=1, keepdims=True))):
                stats = jnp.where(lanes == i * tiles + t, col, stats)
            cols_ref[2, sl] = stats

    def near(g, t0, t1):
        for t in range(t0, t1):
            at = g * tiles + t
            copies.extend(own_sends(t, g))
            arrived(blk(prv, t, g), ids.znxt + at)
            if t % 2 == 0:
                send(blk(prv, t, g), ids.zrel + at, nxt)
            send(blk(prv, t, g), ids.zfp + at, die)
            arrived(blk(nxt, t, g), ids.zprv + at)
            if t % 2 == 1:
                send(blk(nxt, t, g), ids.zrel + at, prv)
            send(blk(nxt, t, g), ids.zfn + at, die)

    for g in range(GROUPS):
        sum_and_send(g)
    finish_sum(0)
    normalize(0)
    for g in range(GROUPS):
        head(g, 0, EARLY)
        if g + 1 < GROUPS:
            finish_sum(g + 1)
        head(g, EARLY, tiles)
        if g + 1 < GROUPS:
            near(g, 0, RELAYED)
            normalize(g + 1)

    by_row = cols_ref[2].T
    tops = by_row[:tiles]
    scale = jnp.exp(tops - jnp.max(tops, axis=0, keepdims=True))
    st_ref[me] = jnp.concatenate(
        [tops, jnp.sum(by_row[tiles:2 * tiles] * scale, axis=0, keepdims=True),
         jnp.sum(by_row[2 * tiles:3 * tiles] * scale, axis=0, keepdims=True),
         jnp.sum(by_row[3 * tiles:4 * tiles], axis=0, keepdims=True),
         jnp.zeros((st_ref.shape[1] - tiles - 3, rows), F32)], axis=0)
    send(st_ref.at[me], ids.snxt, nxt)
    send(st_ref.at[me], ids.sprv, prv)
    send(st_ref.at[me], ids.sopp, opp)
    send(st_ref.at[me], ids.sdie, die)

    for g in range(GROUPS):
        near(g, RELAYED if g + 1 < GROUPS else 0, tiles)

    arrived(st_ref.at[prv], ids.snxt)
    send(st_ref.at[prv], ids.sfp, die)
    arrived(st_ref.at[nxt], ids.sprv)
    send(st_ref.at[nxt], ids.sfn, die)
    arrived(st_ref.at[opp], ids.sopp)
    send(st_ref.at[opp], ids.sfo, die)
    for s, k in ((die, ids.sdie), (p_prv, ids.sfp), (p_nxt, ids.sfn), (p_opp, ids.sfo)):
        arrived(st_ref.at[s], k)

    dev_top = jnp.max(st_ref[:, :tiles], axis=1)
    top = jnp.max(dev_top, axis=0, keepdims=True)
    scale = jnp.exp(dev_top - top)
    sum_exp = jnp.sum(st_ref[:, tiles] * scale, axis=0, keepdims=True)
    weighted = jnp.sum(st_ref[:, tiles + 1] * scale, axis=0, keepdims=True)
    target_logit = jnp.sum(st_ref[:, tiles + 2], axis=0, keepdims=True)
    log_norm = top + jnp.log(sum_exp)
    fin_ref[0:1] = log_norm
    fin_ref[1:2] = log_norm - weighted / sum_exp
    fin_ref[2:3] = target_logit - log_norm
    pad = jnp.zeros((128 - tiles, rows), F32)

    for dev in range(n):
        shift_ref[dev] = jnp.concatenate([st_ref[dev, :tiles] - log_norm, pad], axis=0).T

    ready = []
    for t in range(tiles):
        ready += [("me", me, t), ("prv", prv, t), ("nxt", nxt, t), ("die", die, t), ("p_prv", p_prv, t), ("p_nxt", p_nxt, t)]
    landed = {"die": ids.zdie, "p_prv": ids.zfp, "p_nxt": ids.zfn, "p_opp": ids.zfo}

    def settle(items):
        for name, dev, t in items:
            if name in landed:
                for g in range(GROUPS):
                    arrived(blk(dev, t, g), landed[name] + g * tiles + t)
        for _, dev, t in items:
            b = dev * tiles + t
            z_ref[b] = (raw_ref[b].astype(F32) + shift_ref[dev][:, t:t + 1]).astype(BF16)

    steps = GROUPS * tiles
    taken = 0
    for g in range(GROUPS):
        for t in range(tiles):
            at = g * tiles + t
            upto = max(taken, (at * len(ready)) // (steps - 1))
            batch = ready[taken:upto]
            taken = upto
            if g == GROUPS - 1 and t > 1:
                batch += [("opp", opp, t - 2), ("p_opp", p_opp, t - 2)]
            settle(batch)
            arrived(blk(opp, t, g), ids.zrel + at)
            send(blk(opp, t, g), ids.zfo + at, die)
    settle([("opp", opp, tiles - 2), ("opp", opp, tiles - 1), ("p_opp", p_opp, tiles - 2)])
    settle([("p_opp", p_opp, tiles - 1)])
    for c in copies:
        c.wait_send()


def finish_kernel(z_ref, fin_ref, norm_hbm, ent_hbm, logp_hbm, out_hbm, sem):
    blocks, rows, width = z_ref.shape

    def put(b):
        return pltpu.make_async_copy(
            z_ref.at[b], out_hbm.at[:, pl.ds(pl.multiple_of(b * width, width), width)], sem.at[b])

    @pl.loop(0, blocks)
    def _(b):
        put(b).start()

    small = [pltpu.make_async_copy(fin_ref.at[pl.ds(i, 1)], ref, sem.at[blocks + i])
             for i, ref in enumerate((norm_hbm, ent_hbm, logp_hbm))]
    for c in small:
        c.start()

    @pl.loop(0, blocks)
    def _(b):
        put(b).wait()

    for c in small:
        c.wait()


def solution(mesh):
    n = mesh.shape["tp"]

    def device_step(hidden, w_gate, w_up, w_down, norm_gain, w_vocab, temperature, target):
        rows, dim = hidden.shape
        f_loc = w_gate.shape[1]
        v_loc = w_vocab.shape[1]
        own_w = dim // n
        tiles = v_loc // TILE
        n_ids = Ids(n // 2, tiles).count
        any_spec = pl.BlockSpec(memory_space=pl.ANY)
        vmem = pl.BlockSpec(memory_space=pltpu.VMEM)
        z, fin = pl.pallas_call(
            functools.partial(main_kernel, n),
            out_shape=(pltpu.VMEM((n * tiles, rows, TILE), BF16), pltpu.VMEM((8, rows), F32)),
            in_specs=[any_spec] * 8,
            out_specs=(vmem, vmem),
            scratch_shapes=[
                pltpu.VMEM((v_loc // SLAB, dim, SLAB), BF16),
                pltpu.VMEM((DOWN_SLOTS, f_loc, own_w), BF16),
                pltpu.VMEM((rows, dim), BF16),
                pltpu.VMEM((rows, f_loc), BF16),
                pltpu.VMEM((2, rows, SLAB), F32),
                pltpu.VMEM((1, dim), F32),
                pltpu.VMEM((1, rows), F32),
                pltpu.VMEM((1, rows), jnp.int32),
                pltpu.VMEM((4, rows, own_w), BF16),
                pltpu.VMEM((4, rows, own_w), BF16),
                pltpu.VMEM((3, rows, own_w), BF16),
                pltpu.VMEM((3, rows, own_w), BF16),
                pltpu.VMEM((rows, own_w), F32),
                pltpu.VMEM((n, rows, own_w), BF16),
                pltpu.VMEM((3, rows, 128), F32),
                pltpu.VMEM((n, 16, rows), F32),
                pltpu.VMEM((n, rows, 128), F32),
                pltpu.VMEM((n * tiles, rows, TILE), BF16),
                pltpu.SemaphoreType.DMA((n_ids,)),
                pltpu.SemaphoreType.DMA((n_ids,)),
                pltpu.SemaphoreType.DMA((3, v_loc // SLAB)),
                pltpu.SemaphoreType.DMA((n,)),
                pltpu.SemaphoreType.DMA((4,)),
            ],
            compiler_params=pltpu.CompilerParams(
                collective_id=0, has_side_effects=True, vmem_limit_bytes=57100 * 1024),
            name="decode_tail",
        )(hidden, w_gate, w_up, w_down, norm_gain.reshape(1, dim), w_vocab, temperature.reshape(1, rows),
          target.reshape(1, rows))
        row = jax.ShapeDtypeStruct((1, rows), F32)
        log_norm, entropy, target_logp, log_probs = pl.pallas_call(
            finish_kernel,
            out_shape=(row, row, row, jax.ShapeDtypeStruct((rows, n * v_loc), BF16)),
            in_specs=[vmem, vmem],
            out_specs=(any_spec,) * 4,
            scratch_shapes=[pltpu.SemaphoreType.DMA((n * tiles + 3,))],
            compiler_params=pltpu.CompilerParams(vmem_limit_bytes=4 * 1024 * 1024),
            name="write_log_probs",
        )(z, fin)
        return log_norm.reshape(rows), entropy.reshape(rows), target_logp.reshape(rows), log_probs

    return jax.shard_map(
        device_step,
        mesh=mesh,
        in_specs=(P("dp", None), P(None, "tp"), P(None, "tp"), P("tp", None), P(None),
                  P(None, "tp"), P("dp"), P("dp")),
        out_specs=(P("dp"), P("dp"), P("dp"), P("dp", None)),
        check_vma=False,
    )
```

```python
import functools

import jax
import jax.numpy as jnp
from jax import lax
from jax.experimental import pallas as pl
from jax.experimental.pallas import tpu as pltpu
from jax.sharding import PartitionSpec as P

NORM_EPS = 1e-6
MESH = pl.DeviceIdType.MESH
F32 = jnp.float32
BF16 = jnp.bfloat16

SLAB = 256
AHEAD = 3
DOWN_AHEAD = 3
DOWN_SLOTS = 4
SPLIT = (3, 5)
GROUPS = len(SPLIT)
RELAYED = 6
TILE = 512
FIRST, EARLY = 2, 6


SEND_Y, SEND_Z, SEND_STATS = range(3)


class Ids:
    def __init__(self, chips, tiles):
        self.count = 0
        g = GROUPS
        self.part = self.take(chips)
        self.rs = self.take(g)
        self.ynxt, self.yprv, self.yopp, self.ydie, self.fprv, self.fnxt, self.fopp = (self.take(g) for _ in range(7))
        self.ytop, self.ybot, self.ftop, self.fbot = (self.take(g - 1) for _ in range(4))
        self.znxt, self.zprv, self.zrel = (self.take(g * tiles) for _ in range(3))
        self.zdie, self.zfar = self.take(tiles), self.take(tiles)
        self.snxt, self.sprv, self.sopp, self.sdie, self.sfp, self.sfn, self.sfo = (self.take(1) for _ in range(7))

    def take(self, k):
        first = self.count
        self.count += k
        return first


def main_kernel(n, h_hbm, wg_hbm, wu_hbm, wd_hbm, gain_hbm, wv_hbm, temp_hbm, targ_hbm,
                z_ref, fin_ref,
                wbuf, dbuf, h_ref, a_ref, gu_ref, gain_ref, temp_ref, targ_ref,
                psend, prcv, rsend, rrcv, own_ref, ygat, cols_ref, st_ref, shift_ref, raw_ref,
                ss, rs, wsem, vsem, dsem, msem):
    chips = n // 2
    rows, dim = h_ref.shape
    unit = rows // sum(SPLIT)
    sizes = [unit * k for k in SPLIT]
    starts = [unit * sum(SPLIT[:g]) for g in range(GROUPS)]
    f_loc = a_ref.shape[1]
    nf = f_loc // SLAB
    own_w = dim // n
    tiles = z_ref.shape[0] // n
    per_tile = TILE // SLAB
    ids = Ids(chips, tiles)

    me = lax.axis_index("tp")
    chip, core = me // 2, me % 2
    other = 1 - core
    c_nxt, c_prv, c_opp = (chip + 1) % chips, (chip + chips - 1) % chips, (chip + 2) % chips
    nxt, prv, opp = c_nxt * 2 + core, c_prv * 2 + core, c_opp * 2 + core
    die = chip * 2 + other
    p_prv, p_nxt, p_opp = c_prv * 2 + other, c_nxt * 2 + other, c_opp * 2 + other

    def remote(src, dst, k, dev, kind):
        return pltpu.make_async_remote_copy(src_ref=src, dst_ref=dst, send_sem=ss.at[kind], recv_sem=rs.at[k],
                                            device_id={"tp": dev}, device_id_type=MESH)

    def send(ref, k, dev, kind=SEND_Y):
        remote(ref, ref, k, dev, kind).start()

    def arrived(ref, k):
        remote(ref, ref, k, die, SEND_Y).wait_recv()

    def landed(ref, sem):
        pltpu.make_async_copy(ref, ref, sem).wait()

    def g_rows(g):
        return pl.ds(starts[g], sizes[g])

    def g_slice(g):
        return slice(starts[g], starts[g] + sizes[g])

    small = [pltpu.make_async_copy(h_hbm, h_ref, msem.at[0]),
             pltpu.make_async_copy(gain_hbm, gain_ref, msem.at[1]),
             pltpu.make_async_copy(temp_hbm, temp_ref, msem.at[2]),
             pltpu.make_async_copy(targ_hbm, targ_ref, msem.at[3])]

    def gate_up(j):
        col = pl.ds(pl.multiple_of(j * SLAB, SLAB), SLAB)
        return (pltpu.make_async_copy(wg_hbm.at[:, col], wbuf.at[2 * j], wsem.at[j]),
                pltpu.make_async_copy(wu_hbm.at[:, col], wbuf.at[2 * j + 1], wsem.at[j]))

    def last_pair(part):
        rws = pl.ds(part * (dim // 2), dim // 2)
        col = pl.ds((nf - 1) * SLAB, SLAB)
        return (pltpu.make_async_copy(wg_hbm.at[rws, col], wbuf.at[2 * nf - 2, rws], wsem.at[nf - 1 + part]),
                pltpu.make_async_copy(wu_hbm.at[rws, col], wbuf.at[2 * nf - 1, rws], wsem.at[nf - 1 + part]))

    def start_gate_up(j):
        @pl.when(j < nf - 1)
        def _():
            for c in gate_up(j):
                c.start()

        @pl.when(j == nf - 1)
        def _():
            for c in last_pair(0) + last_pair(1):
                c.start()

    def vocab(s):
        col = pl.ds(pl.multiple_of(s * SLAB, SLAB), SLAB)
        return pltpu.make_async_copy(wv_hbm.at[:, col], wbuf.at[s], vsem.at[s // per_tile])

    def down(k, dev):
        col = pl.ds(pl.multiple_of(dev * own_w, own_w), own_w)
        return pltpu.make_async_copy(wd_hbm.at[:, col], dbuf.at[k % DOWN_SLOTS], dsem.at[k])

    plan = ((c_opp, 0, True), (c_nxt, 1, True), (c_prv, 2, True), (c_opp, 0, False),
            (c_nxt, 1, False), (c_prv, 2, False), (chip, 3, True), (chip, 3, False))
    order = [c * 2 + (other if away else core) for c, _, away in plan]

    small[0].start()
    for j in range(AHEAD):
        start_gate_up(j)
    for c in small[1:]:
        c.start()

    barrier = pltpu.get_barrier_semaphore()
    for r in range(1, n):
        pl.semaphore_signal(barrier, inc=1, device_id={"tp": (me + r) % n}, device_id_type=MESH)

    small[0].wait()
    gu_ref[...] = jnp.zeros_like(gu_ref)

    def activate(j):
        act = jax.nn.silu(gu_ref[0]) * gu_ref[1]
        a_ref[:, pl.ds(pl.multiple_of(j * SLAB, SLAB), SLAB)] = act.astype(BF16)

    @pl.loop(0, nf - 1)
    def _(j):
        landed(wbuf.at[pl.ds(2 * j, 2)], wsem.at[j])

        @pl.when(j + AHEAD < nf)
        def _():
            start_gate_up(j + AHEAD)

        for k in range(DOWN_AHEAD):
            @pl.when(j == nf - AHEAD + min(k, AHEAD - 2))
            def _():
                down(k, order[k]).start()

        activate(jnp.maximum(j - 1, 0))
        gate = jnp.dot(h_ref[...], wbuf[2 * j], preferred_element_type=F32)
        up = jnp.dot(h_ref[...], wbuf[2 * j + 1], preferred_element_type=F32)
        gu_ref[0] = gate
        gu_ref[1] = up

    landed(wbuf.at[pl.ds(2 * nf - 2, 2), pl.ds(0 * (dim // 2), dim // 2)], wsem.at[nf - 1 + 0])
    kh = dim // 2
    activate(nf - 2)
    gu_ref[0] = jnp.dot(h_ref[:, :kh], wbuf[2 * nf - 2, :kh], preferred_element_type=F32)
    gu_ref[1] = jnp.dot(h_ref[:, :kh], wbuf[2 * nf - 1, :kh], preferred_element_type=F32)
    landed(wbuf.at[pl.ds(2 * nf - 2, 2), pl.ds(1 * (dim // 2), dim // 2)], wsem.at[nf - 1 + 1])
    gu_ref[0] += jnp.dot(h_ref[:, kh:], wbuf[2 * nf - 2, kh:], preferred_element_type=F32)
    gu_ref[1] += jnp.dot(h_ref[:, kh:], wbuf[2 * nf - 1, kh:], preferred_element_type=F32)
    activate(nf - 1)

    n_down = len(plan)
    owners = (opp, nxt, prv)

    def reduce_send(q, g):
        remote(rsend.at[q, g_rows(g)], rrcv.at[q, g_rows(g)], ids.rs + g, owners[q], SEND_Y).start()

    for k, (_, q, away) in enumerate(plan):
        if k + DOWN_AHEAD < n_down:
            down(k + DOWN_AHEAD, order[k + DOWN_AHEAD]).start()
        else:
            per = (tiles * per_tile) // DOWN_AHEAD
            first = (k + DOWN_AHEAD - n_down) * per
            last = tiles * per_tile if k == n_down - 1 else first + per
            for s in range(first, last):
                vocab(s).start()
        down(k, order[k]).wait()
        part = jnp.dot(a_ref[...], dbuf[k % DOWN_SLOTS], preferred_element_type=F32)
        to_die = remote(psend.at[q], prcv.at[q], ids.part + q, die, SEND_Y)
        if k == 0:
            pl.semaphore_wait(barrier, n - 1)
        if away:
            psend[q] = part.astype(BF16)
            to_die.start()
            continue
        to_die.wait_recv()
        total = part + prcv[q].astype(F32)
        if q < 3:
            rsend[q] = total.astype(BF16)
            reduce_send(q, 0)
        else:
            own_ref[...] = total
    for g in range(1, GROUPS):
        for q in range(3):
            reduce_send(q, g)

    for c in small[1:]:
        c.wait()
    row_ids = lax.broadcasted_iota(jnp.int32, (rows, rows), 0)
    lane_ids = lax.broadcasted_iota(jnp.int32, (rows, rows), 1)
    eye = row_ids == lane_ids
    inv_temp = 1.0 / jnp.sum(jnp.where(eye, temp_ref[...], 0.0), axis=1, keepdims=True)
    targ = jnp.sum(jnp.where(eye, targ_ref[...].astype(F32), 0.0), axis=1, keepdims=True)
    cols_ref[0] = jnp.broadcast_to(inv_temp, (rows, 128))
    cols_ref[1] = jnp.broadcast_to(targ, (rows, 128))
    cols_ref[2] = jnp.zeros((rows, 128), F32)

    def sum_and_send(g):
        sl = g_slice(g)
        arrived(rrcv.at[:, g_rows(g)], ids.rs + g)
        y = own_ref[sl] + rrcv[0, sl].astype(F32) + rrcv[1, sl].astype(F32) + rrcv[2, sl].astype(F32)
        ygat[me, sl] = y.astype(BF16)
        own = ygat.at[me, g_rows(g)]
        if g == 0:
            send(own, ids.yopp + g, opp)
        send(own, ids.ynxt + g, nxt)
        send(own, ids.yprv + g, prv)
        send(own, ids.ydie + g, die)

    def residual(s, g):
        col = pl.ds(pl.multiple_of(s * own_w, own_w), own_w)
        return col, h_ref[g_rows(g), col].astype(F32) + ygat[s, g_slice(g)].astype(F32)

    def squares(s, g):
        _, r = residual(s, g)
        return jnp.sum(r * r, axis=1, keepdims=True)

    def halves(g):
        top = (sizes[g] // 2 + 15) // 16 * 16
        return pl.ds(starts[g], top), pl.ds(starts[g] + top, sizes[g] - top)

    def forward_near(g):
        for s, k, f in ((prv, ids.ynxt, ids.fprv), (nxt, ids.yprv, ids.fnxt)):
            arrived(ygat.at[s, g_rows(g)], k + g)
            if g > 0 and s is prv:
                send(ygat.at[s, halves(g)[0]], ids.ytop + g - 1, nxt)
            elif g > 0:
                send(ygat.at[s, halves(g)[1]], ids.ybot + g - 1, prv)
            send(ygat.at[s, g_rows(g)], f + g, die)

    def forward_far(g):
        if g == 0:
            arrived(ygat.at[opp, g_rows(g)], ids.yopp + g)
            send(ygat.at[opp, g_rows(g)], ids.fopp + g, die)
            return
        for rws, k, f in zip(halves(g), (ids.ytop, ids.ybot), (ids.ftop, ids.fbot)):
            arrived(ygat.at[opp, rws], k + g - 1)
            send(ygat.at[opp, rws], f + g - 1, die)

    def normalize(g):
        total_sq = squares(me, g) + squares(prv, g) + squares(nxt, g) + squares(opp, g)
        for s, k in ((die, ids.ydie), (p_prv, ids.fprv), (p_nxt, ids.fnxt)):
            arrived(ygat.at[s, g_rows(g)], k + g)
            total_sq += squares(s, g)
        if g == 0:
            arrived(ygat.at[p_opp, g_rows(g)], ids.fopp + g)
        else:
            for rws, k in zip(halves(g), (ids.ftop, ids.fbot)):
                arrived(ygat.at[p_opp, rws], k + g - 1)
        total_sq += squares(p_opp, g)
        inv_rms = lax.rsqrt(total_sq * (1.0 / dim) + NORM_EPS)

        @pl.loop(0, n)
        def _(s):
            col, r = residual(s, g)
            h_ref[g_rows(g), col] = (gain_ref[:, col] * r * inv_rms).astype(BF16)


    def blk(dev, t, g):
        return raw_ref.at[dev * tiles + t, g_rows(g)]

    def own_sends(t, g):
        b = blk(me, t, g)
        at = g * tiles + t
        return (remote(b, b, ids.znxt + at, nxt, SEND_Z), remote(b, b, ids.zprv + at, prv, SEND_Z),
                remote(b, b, ids.zdie + t, die, SEND_Z))

    def head(g, t0, t1):
        sl = g_slice(g)
        lanes = lax.broadcasted_iota(jnp.int32, (sizes[g], 128), 1)

        @pl.loop(t0, t1)
        def _(t):
            if g == 0:
                landed(wbuf.at[pl.ds(t * per_tile, per_tile)], vsem.at[t])
            pieces = [jnp.dot(h_ref[sl], wbuf[t * per_tile + i], preferred_element_type=F32) for i in range(per_tile)]
            logits = jnp.concatenate(pieces, axis=1) * cols_ref[0, sl][:, :1]
            top_l = jnp.max(logits, axis=1, keepdims=True)
            low = logits - top_l
            raw_ref[me * tiles + t, sl] = low.astype(BF16)
            for c in own_sends(t, g):
                c.start()
            e = jnp.exp(low)
            col_ids = lax.broadcasted_iota(jnp.int32, (sizes[g], TILE), 1) + (me * tiles + t) * TILE
            hit = jnp.where(col_ids.astype(F32) == cols_ref[1, sl][:, :1], logits, 0.0)
            stats = cols_ref[2, sl]
            for i, col in enumerate((top_l, jnp.sum(e, axis=1, keepdims=True),
                                     jnp.sum(e * logits, axis=1, keepdims=True), jnp.sum(hit, axis=1, keepdims=True))):
                stats = jnp.where(lanes == i * tiles + t, col, stats)
            cols_ref[2, sl] = stats

    def near(g, t0, t1):
        for t in range(t0, t1):
            at = g * tiles + t
            arrived(blk(prv, t, g), ids.znxt + at)
            if t % 2 == 0:
                send(blk(prv, t, g), ids.zrel + at, nxt, SEND_Z)
            send(blk(prv, t, g), ids.zdie + t, die, SEND_Z)
            arrived(blk(nxt, t, g), ids.zprv + at)
            if t % 2 == 1:
                send(blk(nxt, t, g), ids.zrel + at, prv, SEND_Z)
            send(blk(nxt, t, g), ids.zdie + t, die, SEND_Z)

    for g in range(GROUPS):
        sum_and_send(g)
    forward_near(0)
    forward_far(0)
    normalize(0)
    for g in range(GROUPS):
        more = g + 1 < GROUPS
        head(g, 0, FIRST)
        if more:
            forward_near(g + 1)
        head(g, FIRST, EARLY)
        if more:
            forward_far(g + 1)
        head(g, EARLY, tiles)
        if more:
            near(g, 0, RELAYED)
            normalize(g + 1)

    by_row = cols_ref[2].T
    tops = by_row[:tiles]
    scale = jnp.exp(tops - jnp.max(tops, axis=0, keepdims=True))
    st_ref[me] = jnp.concatenate(
        [tops, jnp.sum(by_row[tiles:2 * tiles] * scale, axis=0, keepdims=True),
         jnp.sum(by_row[2 * tiles:3 * tiles] * scale, axis=0, keepdims=True),
         jnp.sum(by_row[3 * tiles:4 * tiles], axis=0, keepdims=True),
         jnp.zeros((st_ref.shape[1] - tiles - 3, rows), F32)], axis=0)
    send(st_ref.at[me], ids.snxt, nxt, SEND_STATS)
    send(st_ref.at[me], ids.sprv, prv, SEND_STATS)
    send(st_ref.at[me], ids.sopp, opp, SEND_STATS)
    send(st_ref.at[me], ids.sdie, die, SEND_STATS)

    for g in range(GROUPS):
        near(g, RELAYED if g + 1 < GROUPS else 0, tiles)

    arrived(st_ref.at[prv], ids.snxt)
    send(st_ref.at[prv], ids.sfp, die, SEND_STATS)
    arrived(st_ref.at[nxt], ids.sprv)
    send(st_ref.at[nxt], ids.sfn, die, SEND_STATS)
    arrived(st_ref.at[opp], ids.sopp)
    send(st_ref.at[opp], ids.sfo, die, SEND_STATS)
    for s, k in ((die, ids.sdie), (p_prv, ids.sfp), (p_nxt, ids.sfn), (p_opp, ids.sfo)):
        arrived(st_ref.at[s], k)

    dev_top = jnp.max(st_ref[:, :tiles], axis=1)
    top = jnp.max(dev_top, axis=0, keepdims=True)
    scale = jnp.exp(dev_top - top)
    sum_exp = jnp.sum(st_ref[:, tiles] * scale, axis=0, keepdims=True)
    weighted = jnp.sum(st_ref[:, tiles + 1] * scale, axis=0, keepdims=True)
    target_logit = jnp.sum(st_ref[:, tiles + 2], axis=0, keepdims=True)
    log_norm = top + jnp.log(sum_exp)
    fin_ref[0:1] = log_norm
    fin_ref[1:2] = log_norm - weighted / sum_exp
    fin_ref[2:3] = target_logit - log_norm
    pad = jnp.zeros((128 - tiles, rows), F32)

    for dev in range(n):
        shift_ref[dev] = jnp.concatenate([st_ref[dev, :tiles] - log_norm, pad], axis=0).T

    ready = []
    for t in range(tiles):
        ready += [("own", me, t), ("near", prv, t), ("near", nxt, t), ("die", die, t), ("die", p_prv, t), ("die", p_nxt, t)]

    seen = set()

    def settle(items):
        for name, dev, t in items:
            if name == "die" and ("die", t) not in seen:
                arrived(raw_ref.at[pl.ds(0, 3)], ids.zdie + t)
            if name == "far":
                arrived(raw_ref.at[0], ids.zfar + t)
            seen.add((name, t))
        for _, dev, t in items:
            b = dev * tiles + t
            z_ref[b] = (raw_ref[b].astype(F32) + shift_ref[dev][:, t:t + 1]).astype(BF16)

    steps = GROUPS * tiles
    taken = 0
    for g in range(GROUPS):
        for t in range(tiles):
            at = g * tiles + t
            upto = max(taken, (at * len(ready)) // (steps - 1))
            batch = ready[taken:upto]
            taken = upto
            if g == GROUPS - 1 and t > 1:
                batch += [("opp", opp, t - 2), ("far", p_opp, t - 2)]
            settle(batch)
            arrived(blk(opp, t, g), ids.zrel + at)
            send(blk(opp, t, g), ids.zfar + t, die, SEND_Z)
    settle([("opp", opp, tiles - 2), ("opp", opp, tiles - 1), ("far", p_opp, tiles - 2)])
    settle([("far", p_opp, tiles - 1)])
    for ref, kind in ((raw_ref.at[pl.ds(0, 2 * chips + 6)], SEND_Y), (raw_ref.at[pl.ds(0, 7 * tiles)], SEND_Z),
                      (st_ref.at[pl.ds(0, 7)], SEND_STATS)):
        remote(ref, ref, ids.part, die, kind).wait_send()


def finish_kernel(z_ref, fin_ref, norm_hbm, ent_hbm, logp_hbm, out_hbm, sem):
    blocks, rows, width = z_ref.shape

    @pl.loop(0, blocks)
    def _(b):
        pltpu.make_async_copy(
            z_ref.at[b], out_hbm.at[:, pl.ds(pl.multiple_of(b * width, width), width)], sem.at[0]).start()

    for i, ref in enumerate((norm_hbm, ent_hbm, logp_hbm)):
        pltpu.make_async_copy(fin_ref.at[pl.ds(i, 1)], ref, sem.at[1]).start()
    pltpu.make_async_copy(z_ref, z_ref, sem.at[0]).wait()
    pltpu.make_async_copy(fin_ref.at[pl.ds(0, 3)], fin_ref.at[pl.ds(0, 3)], sem.at[1]).wait()


def solution(mesh):
    n = mesh.shape["tp"]

    def device_step(hidden, w_gate, w_up, w_down, norm_gain, w_vocab, temperature, target):
        rows, dim = hidden.shape
        f_loc = w_gate.shape[1]
        v_loc = w_vocab.shape[1]
        own_w = dim // n
        tiles = v_loc // TILE
        n_ids = Ids(n // 2, tiles).count
        any_spec = pl.BlockSpec(memory_space=pl.ANY)
        vmem = pl.BlockSpec(memory_space=pltpu.VMEM)
        z, fin = pl.pallas_call(
            functools.partial(main_kernel, n),
            out_shape=(pltpu.VMEM((n * tiles, rows, TILE), BF16), pltpu.VMEM((8, rows), F32)),
            in_specs=[any_spec] * 8,
            out_specs=(vmem, vmem),
            scratch_shapes=[
                pltpu.VMEM((v_loc // SLAB, dim, SLAB), BF16),
                pltpu.VMEM((DOWN_SLOTS, f_loc, own_w), BF16),
                pltpu.VMEM((rows, dim), BF16),
                pltpu.VMEM((rows, f_loc), BF16),
                pltpu.VMEM((2, rows, SLAB), F32),
                pltpu.VMEM((1, dim), F32),
                pltpu.VMEM((1, rows), F32),
                pltpu.VMEM((1, rows), jnp.int32),
                pltpu.VMEM((4, rows, own_w), BF16),
                pltpu.VMEM((4, rows, own_w), BF16),
                pltpu.VMEM((3, rows, own_w), BF16),
                pltpu.VMEM((3, rows, own_w), BF16),
                pltpu.VMEM((rows, own_w), F32),
                pltpu.VMEM((n, rows, own_w), BF16),
                pltpu.VMEM((3, rows, 128), F32),
                pltpu.VMEM((n, 16, rows), F32),
                pltpu.VMEM((n, rows, 128), F32),
                pltpu.VMEM((n * tiles, rows, TILE), BF16),
                pltpu.SemaphoreType.DMA((3,)),
                pltpu.SemaphoreType.DMA((n_ids,)),
                pltpu.SemaphoreType.DMA((f_loc // SLAB + 1,)),
                pltpu.SemaphoreType.DMA((tiles,)),
                pltpu.SemaphoreType.DMA((n,)),
                pltpu.SemaphoreType.DMA((4,)),
            ],
            compiler_params=pltpu.CompilerParams(
                collective_id=0, has_side_effects=True, vmem_limit_bytes=57100 * 1024),
            name="decode_tail",
        )(hidden, w_gate, w_up, w_down, norm_gain.reshape(1, dim), w_vocab, temperature.reshape(1, rows),
          target.reshape(1, rows))
        row = jax.ShapeDtypeStruct((1, rows), F32)
        log_norm, entropy, target_logp, log_probs = pl.pallas_call(
            finish_kernel,
            out_shape=(row, row, row, jax.ShapeDtypeStruct((rows, n * v_loc), BF16)),
            in_specs=[vmem, vmem],
            out_specs=(any_spec,) * 4,
            scratch_shapes=[pltpu.SemaphoreType.DMA((2,))],
            compiler_params=pltpu.CompilerParams(vmem_limit_bytes=4 * 1024 * 1024),
            name="write_log_probs",
        )(z, fin)
        return log_norm.reshape(rows), entropy.reshape(rows), target_logp.reshape(rows), log_probs

    return jax.shard_map(
        device_step,
        mesh=mesh,
        in_specs=(P("dp", None), P(None, "tp"), P(None, "tp"), P("tp", None), P(None),
                  P(None, "tp"), P("dp"), P("dp")),
        out_specs=(P("dp"), P("dp"), P("dp"), P("dp", None)),
        check_vma=False,
    )
```

```python
import functools

import jax
import jax.numpy as jnp
from jax import lax
from jax.experimental import pallas as pl
from jax.experimental.pallas import tpu as pltpu
from jax.sharding import PartitionSpec as P

NORM_EPS = 1e-6
MESH = pl.DeviceIdType.MESH
F32 = jnp.float32
BF16 = jnp.bfloat16

SLAB = 256
AHEAD = 3
DOWN_AHEAD = 3
DOWN_SLOTS = 4
SPLIT = (3, 5)
GROUPS = len(SPLIT)
RELAYED = (3, 6)
TILE = 512
FIRST, EARLY = 2, 6


SEND_Y, SEND_Z, SEND_STATS = range(3)


class Ids:
    def __init__(self, chips, tiles):
        self.count = 0
        g = GROUPS
        self.part = self.take(chips)
        self.rs = self.take(g)
        self.ynxt, self.yprv, self.yopp, self.ydie = (self.take(g) for _ in range(4))
        self.ytop, self.ybot = (self.take(g - 1) for _ in range(2))
        self.znear = self.take(g * tiles)
        self.zrel = self.take(g * tiles // 2)
        self.zdie, self.zfar = self.take(tiles // 2), self.take(tiles // 2)
        self.stats, self.sdie = self.take(1), self.take(1)

    def take(self, k):
        first = self.count
        self.count += k
        return first


def main_kernel(n, h_hbm, wg_hbm, wu_hbm, wd_hbm, gain_hbm, wv_hbm, temp_hbm, targ_hbm,
                z_ref, fin_ref,
                wbuf, dbuf, h_ref, a_ref, gu_ref, gain_ref, temp_ref, targ_ref,
                psend, prcv, rsend, rrcv, own_ref, ygat, cols_ref, st_ref, shift_ref, raw_ref,
                ss, rs, wsem, vsem, dsem, msem):
    chips = n // 2
    rows, dim = h_ref.shape
    unit = rows // sum(SPLIT)
    sizes = [unit * k for k in SPLIT]
    starts = [unit * sum(SPLIT[:g]) for g in range(GROUPS)]
    f_loc = a_ref.shape[1]
    nf = f_loc // SLAB
    own_w = dim // n
    tiles = z_ref.shape[0] // n
    per_tile = TILE // SLAB
    ids = Ids(chips, tiles)

    me = lax.axis_index("tp")
    chip, core = me // 2, me % 2
    other = 1 - core
    c_nxt, c_prv, c_opp = (chip + 1) % chips, (chip + chips - 1) % chips, (chip + 2) % chips
    nxt, prv, opp = c_nxt * 2 + core, c_prv * 2 + core, c_opp * 2 + core
    die = chip * 2 + other
    p_prv, p_nxt, p_opp = c_prv * 2 + other, c_nxt * 2 + other, c_opp * 2 + other

    def remote(src, dst, k, dev, kind):
        return pltpu.make_async_remote_copy(src_ref=src, dst_ref=dst, send_sem=ss.at[kind], recv_sem=rs.at[k],
                                            device_id={"tp": dev}, device_id_type=MESH)

    def send(ref, k, dev, kind=SEND_Y):
        remote(ref, ref, k, dev, kind).start()

    def arrived(ref, k):
        remote(ref, ref, k, die, SEND_Y).wait_recv()

    def landed(ref, sem):
        pltpu.make_async_copy(ref, ref, sem).wait()

    def g_rows(g):
        return pl.ds(starts[g], sizes[g])

    def g_slice(g):
        return slice(starts[g], starts[g] + sizes[g])

    small = [pltpu.make_async_copy(h_hbm, h_ref, msem.at[0]),
             pltpu.make_async_copy(gain_hbm, gain_ref, msem.at[1]),
             pltpu.make_async_copy(temp_hbm, temp_ref, msem.at[2]),
             pltpu.make_async_copy(targ_hbm, targ_ref, msem.at[3])]

    def gate_up(j):
        col = pl.ds(pl.multiple_of(j * SLAB, SLAB), SLAB)
        return (pltpu.make_async_copy(wg_hbm.at[:, col], wbuf.at[2 * j], wsem.at[j]),
                pltpu.make_async_copy(wu_hbm.at[:, col], wbuf.at[2 * j + 1], wsem.at[j]))

    def last_pair(part):
        rws = pl.ds(part * (dim // 2), dim // 2)
        col = pl.ds((nf - 1) * SLAB, SLAB)
        return (pltpu.make_async_copy(wg_hbm.at[rws, col], wbuf.at[2 * nf - 2, rws], wsem.at[nf - 1 + part]),
                pltpu.make_async_copy(wu_hbm.at[rws, col], wbuf.at[2 * nf - 1, rws], wsem.at[nf - 1 + part]))

    def start_gate_up(j):
        @pl.when(j < nf - 1)
        def _():
            for c in gate_up(j):
                c.start()

        @pl.when(j == nf - 1)
        def _():
            for c in last_pair(0) + last_pair(1):
                c.start()

    def vocab(s):
        col = pl.ds(pl.multiple_of(s * SLAB, SLAB), SLAB)
        return pltpu.make_async_copy(wv_hbm.at[:, col], wbuf.at[s], vsem.at[s // per_tile])

    def down(k, dev):
        col = pl.ds(pl.multiple_of(dev * own_w, own_w), own_w)
        return pltpu.make_async_copy(wd_hbm.at[:, col], dbuf.at[k % DOWN_SLOTS], dsem.at[k % DOWN_SLOTS])

    plan = ((c_opp, 0, True), (c_nxt, 1, True), (c_prv, 2, True), (c_opp, 0, False),
            (c_nxt, 1, False), (c_prv, 2, False), (chip, 3, True), (chip, 3, False))
    order = [c * 2 + (other if away else core) for c, _, away in plan]

    small[0].start()
    for j in range(AHEAD):
        start_gate_up(j)
    for c in small[1:]:
        c.start()

    barrier = pltpu.get_barrier_semaphore()
    for r in range(1, n):
        pl.semaphore_signal(barrier, inc=1, device_id={"tp": (me + r) % n}, device_id_type=MESH)

    small[0].wait()
    gu_ref[...] = jnp.zeros_like(gu_ref)

    def activate(j):
        act = jax.nn.silu(gu_ref[0]) * gu_ref[1]
        a_ref[:, pl.ds(pl.multiple_of(j * SLAB, SLAB), SLAB)] = act.astype(BF16)

    @pl.loop(0, nf - 1)
    def _(j):
        landed(wbuf.at[pl.ds(2 * j, 2)], wsem.at[j])

        @pl.when(j + AHEAD < nf)
        def _():
            start_gate_up(j + AHEAD)

        for k in range(DOWN_AHEAD):
            @pl.when(j == nf - AHEAD + min(k, AHEAD - 2))
            def _():
                down(k, order[k]).start()

        activate(jnp.maximum(j - 1, 0))
        gate = jnp.dot(h_ref[...], wbuf[2 * j], preferred_element_type=F32)
        up = jnp.dot(h_ref[...], wbuf[2 * j + 1], preferred_element_type=F32)
        gu_ref[0] = gate
        gu_ref[1] = up

    landed(wbuf.at[pl.ds(2 * nf - 2, 2), pl.ds(0 * (dim // 2), dim // 2)], wsem.at[nf - 1 + 0])
    kh = dim // 2
    activate(nf - 2)
    gu_ref[0] = jnp.dot(h_ref[:, :kh], wbuf[2 * nf - 2, :kh], preferred_element_type=F32)
    gu_ref[1] = jnp.dot(h_ref[:, :kh], wbuf[2 * nf - 1, :kh], preferred_element_type=F32)
    landed(wbuf.at[pl.ds(2 * nf - 2, 2), pl.ds(1 * (dim // 2), dim // 2)], wsem.at[nf - 1 + 1])
    gu_ref[0] += jnp.dot(h_ref[:, kh:], wbuf[2 * nf - 2, kh:], preferred_element_type=F32)
    gu_ref[1] += jnp.dot(h_ref[:, kh:], wbuf[2 * nf - 1, kh:], preferred_element_type=F32)
    activate(nf - 1)

    n_down = len(plan)
    owners = (opp, nxt, prv)

    def reduce_send(q, g):
        remote(rsend.at[q, g_rows(g)], rrcv.at[q, g_rows(g)], ids.rs + g, owners[q], SEND_Y).start()

    for k, (_, q, away) in enumerate(plan):
        if k + DOWN_AHEAD < n_down:
            down(k + DOWN_AHEAD, order[k + DOWN_AHEAD]).start()
        else:
            per = (tiles * per_tile) // DOWN_AHEAD
            first = (k + DOWN_AHEAD - n_down) * per
            last = tiles * per_tile if k == n_down - 1 else first + per
            for s in range(first, last):
                vocab(s).start()
        down(k, order[k]).wait()
        part = jnp.dot(a_ref[...], dbuf[k % DOWN_SLOTS], preferred_element_type=F32)
        to_die = remote(psend.at[q], prcv.at[q], ids.part + q, die, SEND_Y)
        if k == 0:
            pl.semaphore_wait(barrier, n - 1)
        if away:
            psend[q] = part.astype(BF16)
            to_die.start()
            continue
        to_die.wait_recv()
        total = part + prcv[q].astype(F32)
        if q < 3:
            rsend[q] = total.astype(BF16)
            reduce_send(q, 0)
        else:
            own_ref[...] = total
    for g in range(1, GROUPS):
        for q in range(3):
            reduce_send(q, g)

    for c in small[1:]:
        c.wait()
    row_ids = lax.broadcasted_iota(jnp.int32, (rows, rows), 0)
    lane_ids = lax.broadcasted_iota(jnp.int32, (rows, rows), 1)
    eye = row_ids == lane_ids
    inv_temp = 1.0 / jnp.sum(jnp.where(eye, temp_ref[...], 0.0), axis=1, keepdims=True)
    targ = jnp.sum(jnp.where(eye, targ_ref[...].astype(F32), 0.0), axis=1, keepdims=True)
    cols_ref[0] = jnp.broadcast_to(inv_temp, (rows, 128))
    cols_ref[1] = jnp.broadcast_to(targ, (rows, 128))
    cols_ref[2] = jnp.zeros((rows, 128), F32)

    def sum_and_send(g):
        sl = g_slice(g)
        arrived(rrcv.at[:, g_rows(g)], ids.rs + g)
        y = own_ref[sl] + rrcv[0, sl].astype(F32) + rrcv[1, sl].astype(F32) + rrcv[2, sl].astype(F32)
        ygat[me, sl] = y.astype(BF16)
        own = ygat.at[me, g_rows(g)]
        if g == 0:
            send(own, ids.yopp + g, opp)
        send(own, ids.ynxt + g, nxt)
        send(own, ids.yprv + g, prv)
        send(own, ids.ydie + g, die)

    def residual(s, g):
        col = pl.ds(pl.multiple_of(s * own_w, own_w), own_w)
        return col, h_ref[g_rows(g), col].astype(F32) + ygat[s, g_slice(g)].astype(F32)

    def squares(s, g):
        _, r = residual(s, g)
        return jnp.sum(r * r, axis=1, keepdims=True)

    def halves(g):
        top = (sizes[g] // 2 + 15) // 16 * 16
        return pl.ds(starts[g], top), pl.ds(starts[g] + top, sizes[g] - top)

    def forward_near(g):
        for s, k in ((prv, ids.ynxt), (nxt, ids.yprv)):
            arrived(ygat.at[s, g_rows(g)], k + g)
            if g > 0 and s is prv:
                send(ygat.at[s, halves(g)[0]], ids.ytop + g - 1, nxt)
            elif g > 0:
                send(ygat.at[s, halves(g)[1]], ids.ybot + g - 1, prv)
            send(ygat.at[s, g_rows(g)], ids.ydie + g, die)

    def forward_far(g):
        if g == 0:
            arrived(ygat.at[opp, g_rows(g)], ids.yopp + g)
            send(ygat.at[opp, g_rows(g)], ids.ydie + g, die)
            return
        for rws, k in zip(halves(g), (ids.ytop, ids.ybot)):
            arrived(ygat.at[opp, rws], k + g - 1)
            send(ygat.at[opp, rws], ids.ydie + g, die)

    def normalize(g):
        total_sq = squares(me, g) + squares(prv, g) + squares(nxt, g) + squares(opp, g)
        arrived(ygat.at[pl.ds(0, chips), g_rows(g)], ids.ydie + g)
        for s in (die, p_prv, p_nxt, p_opp):
            total_sq += squares(s, g)
        inv_rms = lax.rsqrt(total_sq * (1.0 / dim) + NORM_EPS)

        @pl.loop(0, n)
        def _(s):
            col, r = residual(s, g)
            h_ref[g_rows(g), col] = (gain_ref[:, col] * r * inv_rms).astype(BF16)


    def blk(dev, t, g):
        return raw_ref.at[dev * tiles + t, g_rows(g)]

    def own_sends(t, g):
        b = blk(me, t, g)
        at = g * tiles + t
        return (remote(b, b, ids.znear + at, nxt, SEND_Z), remote(b, b, ids.znear + at, prv, SEND_Z),
                remote(b, b, ids.zdie + t // 2, die, SEND_Z))

    def head(g, t0, t1):
        sl = g_slice(g)
        lanes = lax.broadcasted_iota(jnp.int32, (sizes[g], 128), 1)

        @pl.loop(t0, t1)
        def _(t):
            if g == 0:
                landed(wbuf.at[pl.ds(t * per_tile, per_tile)], vsem.at[t])
            pieces = [jnp.dot(h_ref[sl], wbuf[t * per_tile + i], preferred_element_type=F32) for i in range(per_tile)]
            logits = jnp.concatenate(pieces, axis=1) * cols_ref[0, sl][:, :1]
            top_l = jnp.max(logits, axis=1, keepdims=True)
            low = logits - top_l
            raw_ref[me * tiles + t, sl] = low.astype(BF16)
            for c in own_sends(t, g):
                c.start()
            e = jnp.exp(low)
            col_ids = lax.broadcasted_iota(jnp.int32, (sizes[g], TILE), 1) + (me * tiles + t) * TILE
            hit = jnp.where(col_ids.astype(F32) == cols_ref[1, sl][:, :1], logits, 0.0)
            stats = cols_ref[2, sl]
            for i, col in enumerate((top_l, jnp.sum(e, axis=1, keepdims=True),
                                     jnp.sum(e * logits, axis=1, keepdims=True), jnp.sum(hit, axis=1, keepdims=True))):
                stats = jnp.where(lanes == i * tiles + t, col, stats)
            cols_ref[2, sl] = stats

    def near(g, t0, t1):
        for t in range(t0, t1):
            at = g * tiles + t
            arrived(raw_ref.at[pl.ds(0, 2), g_rows(g)], ids.znear + at)
            far = (blk(prv, t, g), nxt) if t % 2 == 0 else (blk(nxt, t, g), prv)
            send(far[0], ids.zrel + at // 2, far[1], SEND_Z)
            send(blk(prv, t, g), ids.zdie + t // 2, die, SEND_Z)
            send(blk(nxt, t, g), ids.zdie + t // 2, die, SEND_Z)

    for g in range(GROUPS):
        sum_and_send(g)
    forward_near(0)
    forward_far(0)
    normalize(0)
    for g in range(GROUPS):
        more = g + 1 < GROUPS
        head(g, 0, FIRST)
        if more:
            forward_near(g + 1)
        head(g, FIRST, EARLY)
        if more:
            forward_far(g + 1)
            near(g, 0, RELAYED[0])
        head(g, EARLY, tiles)
        if more:
            near(g, *RELAYED)
            normalize(g + 1)

    by_row = cols_ref[2].T
    tops = by_row[:tiles]
    scale = jnp.exp(tops - jnp.max(tops, axis=0, keepdims=True))
    st_ref[me] = jnp.concatenate(
        [tops, jnp.sum(by_row[tiles:2 * tiles] * scale, axis=0, keepdims=True),
         jnp.sum(by_row[2 * tiles:3 * tiles] * scale, axis=0, keepdims=True),
         jnp.sum(by_row[3 * tiles:4 * tiles], axis=0, keepdims=True),
         jnp.zeros((st_ref.shape[1] - tiles - 3, rows), F32)], axis=0)
    for dev in (nxt, prv, opp):
        send(st_ref.at[me], ids.stats, dev, SEND_STATS)
    send(st_ref.at[me], ids.sdie, die, SEND_STATS)

    for g in range(GROUPS):
        near(g, RELAYED[1] if g + 1 < GROUPS else 0, tiles)

    arrived(st_ref.at[pl.ds(0, 3)], ids.stats)
    for dev in (prv, nxt, opp):
        send(st_ref.at[dev], ids.sdie, die, SEND_STATS)
    arrived(st_ref.at[pl.ds(0, chips)], ids.sdie)

    dev_top = jnp.max(st_ref[:, :tiles], axis=1)
    top = jnp.max(dev_top, axis=0, keepdims=True)
    scale = jnp.exp(dev_top - top)
    sum_exp = jnp.sum(st_ref[:, tiles] * scale, axis=0, keepdims=True)
    weighted = jnp.sum(st_ref[:, tiles + 1] * scale, axis=0, keepdims=True)
    target_logit = jnp.sum(st_ref[:, tiles + 2], axis=0, keepdims=True)
    log_norm = top + jnp.log(sum_exp)
    fin_ref[0:1] = log_norm
    fin_ref[1:2] = log_norm - weighted / sum_exp
    fin_ref[2:3] = target_logit - log_norm
    pad = jnp.zeros((128 - tiles, rows), F32)

    for dev in range(n):
        shift_ref[dev] = jnp.concatenate([st_ref[dev, :tiles] - log_norm, pad], axis=0).T

    ready = []
    for t in range(tiles):
        ready += [("own", me, t), ("near", prv, t), ("near", nxt, t), ("die", die, t), ("die", p_prv, t), ("die", p_nxt, t)]

    seen = set()

    def settle(items):
        for name, dev, t in items:
            key = (name, t // 2)
            if name == "die" and key not in seen:
                arrived(raw_ref.at[pl.ds(0, 6)], ids.zdie + t // 2)
            if name == "far" and key not in seen:
                arrived(raw_ref.at[pl.ds(0, 2)], ids.zfar + t // 2)
            seen.add(key)
        for _, dev, t in items:
            b = dev * tiles + t
            z_ref[b] = (raw_ref[b].astype(F32) + shift_ref[dev][:, t:t + 1]).astype(BF16)

    pairs = tiles // 2
    steps = GROUPS * pairs
    taken = 0
    for g in range(GROUPS):
        for p in range(pairs):
            at = g * pairs + p
            upto = max(taken, (at * len(ready)) // (steps - 1))
            batch = ready[taken:upto]
            taken = upto
            for i in range(0, len(batch), 3):
                settle(batch[i:i + 3])
            if g == GROUPS - 1 and p > 1:
                settle([(name, dev, 2 * p - 4 + i) for name, dev in (("opp", opp), ("far", p_opp)) for i in range(2)])
            arrived(raw_ref.at[pl.ds(0, 2), g_rows(g)], ids.zrel + at)
            for t in (2 * p, 2 * p + 1):
                send(blk(opp, t, g), ids.zfar + p, die, SEND_Z)
    settle([("opp", opp, tiles - 4 + i) for i in range(4)])
    settle([("far", p_opp, tiles - 4 + i) for i in range(2)])
    settle([("far", p_opp, tiles - 2 + i) for i in range(2)])
    for ref, kind in ((raw_ref.at[pl.ds(0, 2 * chips + 6)], SEND_Y), (raw_ref.at[pl.ds(0, 7 * tiles)], SEND_Z),
                      (st_ref.at[pl.ds(0, 7)], SEND_STATS)):
        remote(ref, ref, ids.part, die, kind).wait_send()


def finish_kernel(z_ref, fin_ref, norm_hbm, ent_hbm, logp_hbm, out_hbm, sem):
    blocks, rows, width = z_ref.shape

    @pl.loop(0, blocks)
    def _(b):
        pltpu.make_async_copy(
            z_ref.at[b], out_hbm.at[:, pl.ds(pl.multiple_of(b * width, width), width)], sem.at[0]).start()

    for i, ref in enumerate((norm_hbm, ent_hbm, logp_hbm)):
        pltpu.make_async_copy(fin_ref.at[pl.ds(i, 1)], ref, sem.at[1]).start()
    pltpu.make_async_copy(z_ref, z_ref, sem.at[0]).wait()
    pltpu.make_async_copy(fin_ref.at[pl.ds(0, 3)], fin_ref.at[pl.ds(0, 3)], sem.at[1]).wait()


def solution(mesh):
    n = mesh.shape["tp"]

    def device_step(hidden, w_gate, w_up, w_down, norm_gain, w_vocab, temperature, target):
        rows, dim = hidden.shape
        f_loc = w_gate.shape[1]
        v_loc = w_vocab.shape[1]
        own_w = dim // n
        tiles = v_loc // TILE
        n_ids = Ids(n // 2, tiles).count
        any_spec = pl.BlockSpec(memory_space=pl.ANY)
        vmem = pl.BlockSpec(memory_space=pltpu.VMEM)
        z, fin = pl.pallas_call(
            functools.partial(main_kernel, n),
            out_shape=(pltpu.VMEM((n * tiles, rows, TILE), BF16), pltpu.VMEM((8, rows), F32)),
            in_specs=[any_spec] * 8,
            out_specs=(vmem, vmem),
            scratch_shapes=[
                pltpu.VMEM((v_loc // SLAB, dim, SLAB), BF16),
                pltpu.VMEM((DOWN_SLOTS, f_loc, own_w), BF16),
                pltpu.VMEM((rows, dim), BF16),
                pltpu.VMEM((rows, f_loc), BF16),
                pltpu.VMEM((2, rows, SLAB), F32),
                pltpu.VMEM((1, dim), F32),
                pltpu.VMEM((1, rows), F32),
                pltpu.VMEM((1, rows), jnp.int32),
                pltpu.VMEM((4, rows, own_w), BF16),
                pltpu.VMEM((4, rows, own_w), BF16),
                pltpu.VMEM((3, rows, own_w), BF16),
                pltpu.VMEM((3, rows, own_w), BF16),
                pltpu.VMEM((rows, own_w), F32),
                pltpu.VMEM((n, rows, own_w), BF16),
                pltpu.VMEM((3, rows, 128), F32),
                pltpu.VMEM((n, 16, rows), F32),
                pltpu.VMEM((n, rows, 128), F32),
                pltpu.VMEM((n * tiles, rows, TILE), BF16),
                pltpu.SemaphoreType.DMA((3,)),
                pltpu.SemaphoreType.DMA((n_ids,)),
                pltpu.SemaphoreType.DMA((f_loc // SLAB + 1,)),
                pltpu.SemaphoreType.DMA((tiles,)),
                pltpu.SemaphoreType.DMA((DOWN_SLOTS,)),
                pltpu.SemaphoreType.DMA((4,)),
            ],
            compiler_params=pltpu.CompilerParams(
                collective_id=0, has_side_effects=True, vmem_limit_bytes=57100 * 1024),
            name="decode_tail",
        )(hidden, w_gate, w_up, w_down, norm_gain.reshape(1, dim), w_vocab, temperature.reshape(1, rows),
          target.reshape(1, rows))
        row = jax.ShapeDtypeStruct((1, rows), F32)
        log_norm, entropy, target_logp, log_probs = pl.pallas_call(
            finish_kernel,
            out_shape=(row, row, row, jax.ShapeDtypeStruct((rows, n * v_loc), BF16)),
            in_specs=[vmem, vmem],
            out_specs=(any_spec,) * 4,
            scratch_shapes=[pltpu.SemaphoreType.DMA((2,))],
            compiler_params=pltpu.CompilerParams(vmem_limit_bytes=4 * 1024 * 1024),
            name="write_log_probs",
        )(z, fin)
        return log_norm.reshape(rows), entropy.reshape(rows), target_logp.reshape(rows), log_probs

    return jax.shard_map(
        device_step,
        mesh=mesh,
        in_specs=(P("dp", None), P(None, "tp"), P(None, "tp"), P("tp", None), P(None),
                  P(None, "tp"), P("dp"), P("dp")),
        out_specs=(P("dp"), P("dp"), P("dp"), P("dp", None)),
        check_vma=False,
    )
```

```python
import functools

import jax
import jax.numpy as jnp
from jax import lax
from jax.experimental import pallas as pl
from jax.experimental.pallas import tpu as pltpu
from jax.sharding import PartitionSpec as P

NORM_EPS = 1e-6
MESH = pl.DeviceIdType.MESH
F32 = jnp.float32
BF16 = jnp.bfloat16

SLAB = 256
AHEAD = 3
DOWN_AHEAD = 3
DOWN_SLOTS = 4
SPLIT = (4, 4)
GROUPS = len(SPLIT)
RELAYED = (3, 6)
TILE = 512
FIRST, EARLY = 2, 6


SEND_Y, SEND_Z, SEND_STATS = range(3)


class Ids:
    def __init__(self, chips, tiles):
        self.count = 0
        g = GROUPS
        self.part = self.take(chips)
        self.rs = self.take(g)
        self.ynxt, self.yprv, self.yopp, self.ydie = (self.take(g) for _ in range(4))
        self.ytop, self.ybot = (self.take(g - 1) for _ in range(2))
        self.znear = self.take(g * tiles)
        self.zrel = self.take(g * tiles // 2)
        self.zdie, self.zfar = self.take(tiles // 2), self.take(tiles // 2)
        self.stats, self.sdie = self.take(1), self.take(1)

    def take(self, k):
        first = self.count
        self.count += k
        return first


def main_kernel(n, h_hbm, wg_hbm, wu_hbm, wd_hbm, gain_hbm, wv_hbm, temp_hbm, targ_hbm,
                z_ref, fin_ref,
                wbuf, dbuf, h_ref, a_ref, gu_ref, gain_ref, temp_ref, targ_ref,
                psend, prcv, rsend, rrcv, own_ref, ygat, cols_ref, st_ref, shift_ref, raw_ref,
                ss, rs, wsem, vsem, dsem, msem):
    chips = n // 2
    rows, dim = h_ref.shape
    unit = rows // sum(SPLIT)
    sizes = [unit * k for k in SPLIT]
    starts = [unit * sum(SPLIT[:g]) for g in range(GROUPS)]
    f_loc = a_ref.shape[1]
    nf = f_loc // SLAB
    own_w = dim // n
    tiles = z_ref.shape[0] // n
    per_tile = TILE // SLAB
    ids = Ids(chips, tiles)

    me = lax.axis_index("tp")
    chip, core = me // 2, me % 2
    other = 1 - core
    c_nxt, c_prv, c_opp = (chip + 1) % chips, (chip + chips - 1) % chips, (chip + 2) % chips
    nxt, prv, opp = c_nxt * 2 + core, c_prv * 2 + core, c_opp * 2 + core
    die = chip * 2 + other
    p_prv, p_nxt, p_opp = c_prv * 2 + other, c_nxt * 2 + other, c_opp * 2 + other

    def remote(src, dst, k, dev, kind):
        return pltpu.make_async_remote_copy(src_ref=src, dst_ref=dst, send_sem=ss.at[kind], recv_sem=rs.at[k],
                                            device_id={"tp": dev}, device_id_type=MESH)

    def send(ref, k, dev, kind=SEND_Y):
        remote(ref, ref, k, dev, kind).start()

    def arrived(ref, k):
        remote(ref, ref, k, die, SEND_Y).wait_recv()

    def landed(ref, sem):
        pltpu.make_async_copy(ref, ref, sem).wait()

    def g_rows(g):
        return pl.ds(starts[g], sizes[g])

    def g_slice(g):
        return slice(starts[g], starts[g] + sizes[g])

    small = [pltpu.make_async_copy(h_hbm, h_ref, msem.at[0]),
             pltpu.make_async_copy(gain_hbm, gain_ref, msem.at[1]),
             pltpu.make_async_copy(temp_hbm, temp_ref, msem.at[2]),
             pltpu.make_async_copy(targ_hbm, targ_ref, msem.at[3])]

    def gate_up(j):
        col = pl.ds(pl.multiple_of(j * SLAB, SLAB), SLAB)
        return (pltpu.make_async_copy(wg_hbm.at[:, col], wbuf.at[2 * j], wsem.at[j]),
                pltpu.make_async_copy(wu_hbm.at[:, col], wbuf.at[2 * j + 1], wsem.at[j]))

    def last_pair(part):
        rws = pl.ds(part * (dim // 2), dim // 2)
        col = pl.ds((nf - 1) * SLAB, SLAB)
        return (pltpu.make_async_copy(wg_hbm.at[rws, col], wbuf.at[2 * nf - 2, rws], wsem.at[nf - 1 + part]),
                pltpu.make_async_copy(wu_hbm.at[rws, col], wbuf.at[2 * nf - 1, rws], wsem.at[nf - 1 + part]))

    def start_gate_up(j):
        @pl.when(j < nf - 1)
        def _():
            for c in gate_up(j):
                c.start()

        @pl.when(j == nf - 1)
        def _():
            for c in last_pair(0) + last_pair(1):
                c.start()

    def vocab(s):
        col = pl.ds(pl.multiple_of(s * SLAB, SLAB), SLAB)
        return pltpu.make_async_copy(wv_hbm.at[:, col], wbuf.at[s], vsem.at[s // per_tile])

    def down(k, dev):
        col = pl.ds(pl.multiple_of(dev * own_w, own_w), own_w)
        return pltpu.make_async_copy(wd_hbm.at[:, col], dbuf.at[k % DOWN_SLOTS], dsem.at[k % DOWN_SLOTS])

    plan = ((c_opp, 0, True), (c_nxt, 1, True), (c_prv, 2, True), (c_opp, 0, False),
            (c_nxt, 1, False), (c_prv, 2, False), (chip, 3, True), (chip, 3, False))
    order = [c * 2 + (other if away else core) for c, _, away in plan]

    small[0].start()
    for j in range(AHEAD):
        start_gate_up(j)
    for c in small[1:]:
        c.start()

    barrier = pltpu.get_barrier_semaphore()
    for r in range(1, n):
        pl.semaphore_signal(barrier, inc=1, device_id={"tp": (me + r) % n}, device_id_type=MESH)

    small[0].wait()
    gu_ref[...] = jnp.zeros_like(gu_ref)

    def activate(j):
        act = jax.nn.silu(gu_ref[0]) * gu_ref[1]
        a_ref[:, pl.ds(pl.multiple_of(j * SLAB, SLAB), SLAB)] = act.astype(BF16)

    @pl.loop(0, nf - 1)
    def _(j):
        landed(wbuf.at[pl.ds(2 * j, 2)], wsem.at[j])

        @pl.when(j + AHEAD < nf)
        def _():
            start_gate_up(j + AHEAD)

        for k in range(DOWN_AHEAD):
            @pl.when(j == nf - AHEAD + min(k, AHEAD - 2))
            def _():
                down(k, order[k]).start()

        activate(jnp.maximum(j - 1, 0))
        gate = jnp.dot(h_ref[...], wbuf[2 * j], preferred_element_type=F32)
        up = jnp.dot(h_ref[...], wbuf[2 * j + 1], preferred_element_type=F32)
        gu_ref[0] = gate
        gu_ref[1] = up

    landed(wbuf.at[pl.ds(2 * nf - 2, 2), pl.ds(0 * (dim // 2), dim // 2)], wsem.at[nf - 1 + 0])
    kh = dim // 2
    activate(nf - 2)
    gu_ref[0] = jnp.dot(h_ref[:, :kh], wbuf[2 * nf - 2, :kh], preferred_element_type=F32)
    gu_ref[1] = jnp.dot(h_ref[:, :kh], wbuf[2 * nf - 1, :kh], preferred_element_type=F32)
    landed(wbuf.at[pl.ds(2 * nf - 2, 2), pl.ds(1 * (dim // 2), dim // 2)], wsem.at[nf - 1 + 1])
    gu_ref[0] += jnp.dot(h_ref[:, kh:], wbuf[2 * nf - 2, kh:], preferred_element_type=F32)
    gu_ref[1] += jnp.dot(h_ref[:, kh:], wbuf[2 * nf - 1, kh:], preferred_element_type=F32)
    activate(nf - 1)

    n_down = len(plan)
    owners = (opp, nxt, prv)

    def reduce_send(q, g):
        remote(rsend.at[q, g_rows(g)], rrcv.at[q, g_rows(g)], ids.rs + g, owners[q], SEND_Y).start()

    for k, (_, q, away) in enumerate(plan):
        if k + DOWN_AHEAD < n_down:
            down(k + DOWN_AHEAD, order[k + DOWN_AHEAD]).start()
        else:
            per = (tiles * per_tile) // DOWN_AHEAD
            first = (k + DOWN_AHEAD - n_down) * per
            last = tiles * per_tile if k == n_down - 1 else first + per
            for s in range(first, last):
                vocab(s).start()
        down(k, order[k]).wait()
        part = jnp.dot(a_ref[...], dbuf[k % DOWN_SLOTS], preferred_element_type=F32)
        to_die = remote(psend.at[q], prcv.at[q], ids.part + q, die, SEND_Y)
        if k == 0:
            pl.semaphore_wait(barrier, n - 1)
        if away:
            psend[q] = part.astype(BF16)
            to_die.start()
            continue
        to_die.wait_recv()
        total = part + prcv[q].astype(F32)
        if q < 3:
            rsend[q] = total.astype(BF16)
            reduce_send(q, 0)
            if q == 2:
                for g in range(1, GROUPS):
                    for r in range(3):
                        reduce_send(r, g)
        else:
            own_ref[...] = total
    for c in small[1:]:
        c.wait()
    row_ids = lax.broadcasted_iota(jnp.int32, (rows, rows), 0)
    lane_ids = lax.broadcasted_iota(jnp.int32, (rows, rows), 1)
    eye = row_ids == lane_ids
    inv_temp = 1.0 / jnp.sum(jnp.where(eye, temp_ref[...], 0.0), axis=1, keepdims=True)
    targ = jnp.sum(jnp.where(eye, targ_ref[...].astype(F32), 0.0), axis=1, keepdims=True)
    cols_ref[0] = jnp.broadcast_to(inv_temp, (rows, 128))
    cols_ref[1] = jnp.broadcast_to(targ, (rows, 128))
    cols_ref[2] = jnp.zeros((rows, 128), F32)

    def sum_and_send(g):
        sl = g_slice(g)
        arrived(rrcv.at[:, g_rows(g)], ids.rs + g)
        y = own_ref[sl] + rrcv[0, sl].astype(F32) + rrcv[1, sl].astype(F32) + rrcv[2, sl].astype(F32)
        ygat[me, sl] = y.astype(BF16)
        own = ygat.at[me, g_rows(g)]
        if g == 0:
            send(own, ids.yopp + g, opp)
        send(own, ids.ynxt + g, nxt)
        send(own, ids.yprv + g, prv)
        send(own, ids.ydie + g, die)

    def residual(s, g):
        col = pl.ds(pl.multiple_of(s * own_w, own_w), own_w)
        return col, h_ref[g_rows(g), col].astype(F32) + ygat[s, g_slice(g)].astype(F32)

    def squares(s, g):
        _, r = residual(s, g)
        return jnp.sum(r * r, axis=1, keepdims=True)

    def halves(g):
        top = (sizes[g] // 2 + 15) // 16 * 16
        return pl.ds(starts[g], top), pl.ds(starts[g] + top, sizes[g] - top)

    def forward_near(g):
        for s, k in ((prv, ids.ynxt), (nxt, ids.yprv)):
            arrived(ygat.at[s, g_rows(g)], k + g)
            if g > 0 and s is prv:
                send(ygat.at[s, halves(g)[0]], ids.ytop + g - 1, nxt)
            elif g > 0:
                send(ygat.at[s, halves(g)[1]], ids.ybot + g - 1, prv)
            send(ygat.at[s, g_rows(g)], ids.ydie + g, die)

    def forward_far(g):
        if g == 0:
            arrived(ygat.at[opp, g_rows(g)], ids.yopp + g)
            send(ygat.at[opp, g_rows(g)], ids.ydie + g, die)
            return
        for rws, k in zip(halves(g), (ids.ytop, ids.ybot)):
            arrived(ygat.at[opp, rws], k + g - 1)
            send(ygat.at[opp, rws], ids.ydie + g, die)

    def normalize(g):
        total_sq = squares(me, g) + squares(prv, g) + squares(nxt, g) + squares(opp, g)
        arrived(ygat.at[pl.ds(0, chips), g_rows(g)], ids.ydie + g)
        for s in (die, p_prv, p_nxt, p_opp):
            total_sq += squares(s, g)
        inv_rms = lax.rsqrt(total_sq * (1.0 / dim) + NORM_EPS)

        @pl.loop(0, n)
        def _(s):
            col, r = residual(s, g)
            h_ref[g_rows(g), col] = (gain_ref[:, col] * r * inv_rms).astype(BF16)


    def blk(dev, t, g):
        return raw_ref.at[dev * tiles + t, g_rows(g)]

    def own_sends(t, g):
        b = blk(me, t, g)
        at = g * tiles + t
        return (remote(b, b, ids.znear + at, nxt, SEND_Z), remote(b, b, ids.znear + at, prv, SEND_Z),
                remote(b, b, ids.zdie + t // 2, die, SEND_Z))

    def head(g, t0, t1):
        sl = g_slice(g)
        lanes = lax.broadcasted_iota(jnp.int32, (sizes[g], 128), 1)

        @pl.loop(t0, t1)
        def _(t):
            if g == 0:
                landed(wbuf.at[pl.ds(t * per_tile, per_tile)], vsem.at[t])
            pieces = [jnp.dot(h_ref[sl], wbuf[t * per_tile + i], preferred_element_type=F32) for i in range(per_tile)]
            logits = jnp.concatenate(pieces, axis=1) * cols_ref[0, sl][:, :1]
            top_l = jnp.max(logits, axis=1, keepdims=True)
            low = logits - top_l
            raw_ref[me * tiles + t, sl] = low.astype(BF16)
            for c in own_sends(t, g):
                c.start()
            e = jnp.exp(low)
            col_ids = lax.broadcasted_iota(jnp.int32, (sizes[g], TILE), 1) + (me * tiles + t) * TILE
            hit = jnp.where(col_ids.astype(F32) == cols_ref[1, sl][:, :1], logits, 0.0)
            stats = cols_ref[2, sl]
            for i, col in enumerate((top_l, jnp.sum(e, axis=1, keepdims=True),
                                     jnp.sum(e * logits, axis=1, keepdims=True), jnp.sum(hit, axis=1, keepdims=True))):
                stats = jnp.where(lanes == i * tiles + t, col, stats)
            cols_ref[2, sl] = stats

    def near(g, t0, t1):
        for t in range(t0, t1):
            at = g * tiles + t
            arrived(raw_ref.at[pl.ds(0, 2), g_rows(g)], ids.znear + at)
            far = (blk(prv, t, g), nxt) if t % 2 == 0 else (blk(nxt, t, g), prv)
            send(far[0], ids.zrel + at // 2, far[1], SEND_Z)
            send(blk(prv, t, g), ids.zdie + t // 2, die, SEND_Z)
            send(blk(nxt, t, g), ids.zdie + t // 2, die, SEND_Z)

    for g in range(GROUPS):
        sum_and_send(g)
    forward_near(0)
    forward_far(0)
    normalize(0)
    for g in range(GROUPS):
        more = g + 1 < GROUPS
        head(g, 0, FIRST)
        if more:
            forward_near(g + 1)
        head(g, FIRST, EARLY)
        if more:
            forward_far(g + 1)
            near(g, 0, RELAYED[0])
        head(g, EARLY, tiles)
        if more:
            near(g, *RELAYED)
            normalize(g + 1)

    by_row = cols_ref[2].T
    tops = by_row[:tiles]
    scale = jnp.exp(tops - jnp.max(tops, axis=0, keepdims=True))
    st_ref[me] = jnp.concatenate(
        [tops, jnp.sum(by_row[tiles:2 * tiles] * scale, axis=0, keepdims=True),
         jnp.sum(by_row[2 * tiles:3 * tiles] * scale, axis=0, keepdims=True),
         jnp.sum(by_row[3 * tiles:4 * tiles], axis=0, keepdims=True),
         jnp.zeros((st_ref.shape[1] - tiles - 3, rows), F32)], axis=0)
    for dev in (nxt, prv, opp):
        send(st_ref.at[me], ids.stats, dev, SEND_STATS)
    send(st_ref.at[me], ids.sdie, die, SEND_STATS)

    for g in range(GROUPS):
        near(g, RELAYED[1] if g + 1 < GROUPS else 0, tiles)

    arrived(st_ref.at[pl.ds(0, 3)], ids.stats)
    for dev in (prv, nxt, opp):
        send(st_ref.at[dev], ids.sdie, die, SEND_STATS)
    arrived(st_ref.at[pl.ds(0, chips)], ids.sdie)

    dev_top = jnp.max(st_ref[:, :tiles], axis=1)
    top = jnp.max(dev_top, axis=0, keepdims=True)
    scale = jnp.exp(dev_top - top)
    sum_exp = jnp.sum(st_ref[:, tiles] * scale, axis=0, keepdims=True)
    weighted = jnp.sum(st_ref[:, tiles + 1] * scale, axis=0, keepdims=True)
    target_logit = jnp.sum(st_ref[:, tiles + 2], axis=0, keepdims=True)
    log_norm = top + jnp.log(sum_exp)
    fin_ref[0:1] = log_norm
    fin_ref[1:2] = log_norm - weighted / sum_exp
    fin_ref[2:3] = target_logit - log_norm
    pad = jnp.zeros((128 - tiles, rows), F32)

    for dev in range(n):
        shift_ref[dev] = jnp.concatenate([st_ref[dev, :tiles] - log_norm, pad], axis=0).T

    ready = []
    for t in range(tiles):
        ready += [("own", me, t), ("near", prv, t), ("near", nxt, t), ("die", die, t), ("die", p_prv, t), ("die", p_nxt, t)]

    seen = set()

    def settle(items):
        for name, dev, t in items:
            key = (name, t // 2)
            if name == "die" and key not in seen:
                arrived(raw_ref.at[pl.ds(0, 6)], ids.zdie + t // 2)
            if name == "far" and key not in seen:
                arrived(raw_ref.at[pl.ds(0, 2)], ids.zfar + t // 2)
            seen.add(key)
        for _, dev, t in items:
            b = dev * tiles + t
            z_ref[b] = (raw_ref[b].astype(F32) + shift_ref[dev][:, t:t + 1]).astype(BF16)

    pairs = tiles // 2
    steps = GROUPS * pairs
    taken = 0
    for g in range(GROUPS):
        for p in range(pairs):
            at = g * pairs + p
            upto = max(taken, (at * len(ready)) // (steps - 1))
            batch = ready[taken:upto]
            taken = upto
            for i in range(0, len(batch), 3):
                settle(batch[i:i + 3])
            if g == GROUPS - 1 and p > 1:
                settle([(name, dev, 2 * p - 4 + i) for name, dev in (("opp", opp), ("far", p_opp)) for i in range(2)])
            arrived(raw_ref.at[pl.ds(0, 2), g_rows(g)], ids.zrel + at)
            for t in (2 * p, 2 * p + 1):
                send(blk(opp, t, g), ids.zfar + p, die, SEND_Z)
    settle([("opp", opp, tiles - 4 + i) for i in range(4)])
    settle([("far", p_opp, tiles - 4 + i) for i in range(2)])
    settle([("far", p_opp, tiles - 2 + i) for i in range(2)])
    for ref, kind in ((raw_ref.at[pl.ds(0, 2 * chips + 6)], SEND_Y), (raw_ref.at[pl.ds(0, 7 * tiles)], SEND_Z),
                      (st_ref.at[pl.ds(0, 7)], SEND_STATS)):
        remote(ref, ref, ids.part, die, kind).wait_send()


def finish_kernel(z_ref, fin_ref, norm_hbm, ent_hbm, logp_hbm, out_hbm, sem):
    blocks, rows, width = z_ref.shape

    @pl.loop(0, blocks)
    def _(b):
        pltpu.make_async_copy(
            z_ref.at[b], out_hbm.at[:, pl.ds(pl.multiple_of(b * width, width), width)], sem.at[0]).start()

    for i, ref in enumerate((norm_hbm, ent_hbm, logp_hbm)):
        pltpu.make_async_copy(fin_ref.at[pl.ds(i, 1)], ref, sem.at[1]).start()
    pltpu.make_async_copy(z_ref, z_ref, sem.at[0]).wait()
    pltpu.make_async_copy(fin_ref.at[pl.ds(0, 3)], fin_ref.at[pl.ds(0, 3)], sem.at[1]).wait()


def solution(mesh):
    n = mesh.shape["tp"]

    def device_step(hidden, w_gate, w_up, w_down, norm_gain, w_vocab, temperature, target):
        rows, dim = hidden.shape
        f_loc = w_gate.shape[1]
        v_loc = w_vocab.shape[1]
        own_w = dim // n
        tiles = v_loc // TILE
        n_ids = Ids(n // 2, tiles).count
        any_spec = pl.BlockSpec(memory_space=pl.ANY)
        vmem = pl.BlockSpec(memory_space=pltpu.VMEM)
        z, fin = pl.pallas_call(
            functools.partial(main_kernel, n),
            out_shape=(pltpu.VMEM((n * tiles, rows, TILE), BF16), pltpu.VMEM((8, rows), F32)),
            in_specs=[any_spec] * 8,
            out_specs=(vmem, vmem),
            scratch_shapes=[
                pltpu.VMEM((v_loc // SLAB, dim, SLAB), BF16),
                pltpu.VMEM((DOWN_SLOTS, f_loc, own_w), BF16),
                pltpu.VMEM((rows, dim), BF16),
                pltpu.VMEM((rows, f_loc), BF16),
                pltpu.VMEM((2, rows, SLAB), F32),
                pltpu.VMEM((1, dim), F32),
                pltpu.VMEM((1, rows), F32),
                pltpu.VMEM((1, rows), jnp.int32),
                pltpu.VMEM((4, rows, own_w), BF16),
                pltpu.VMEM((4, rows, own_w), BF16),
                pltpu.VMEM((3, rows, own_w), BF16),
                pltpu.VMEM((3, rows, own_w), BF16),
                pltpu.VMEM((rows, own_w), F32),
                pltpu.VMEM((n, rows, own_w), BF16),
                pltpu.VMEM((3, rows, 128), F32),
                pltpu.VMEM((n, 16, rows), F32),
                pltpu.VMEM((n, rows, 128), F32),
                pltpu.VMEM((n * tiles, rows, TILE), BF16),
                pltpu.SemaphoreType.DMA((3,)),
                pltpu.SemaphoreType.DMA((n_ids,)),
                pltpu.SemaphoreType.DMA((f_loc // SLAB + 1,)),
                pltpu.SemaphoreType.DMA((tiles,)),
                pltpu.SemaphoreType.DMA((DOWN_SLOTS,)),
                pltpu.SemaphoreType.DMA((4,)),
            ],
            compiler_params=pltpu.CompilerParams(
                collective_id=0, has_side_effects=True, vmem_limit_bytes=57100 * 1024),
            name="decode_tail",
        )(hidden, w_gate, w_up, w_down, norm_gain.reshape(1, dim), w_vocab, temperature.reshape(1, rows),
          target.reshape(1, rows))
        row = jax.ShapeDtypeStruct((1, rows), F32)
        log_norm, entropy, target_logp, log_probs = pl.pallas_call(
            finish_kernel,
            out_shape=(row, row, row, jax.ShapeDtypeStruct((rows, n * v_loc), BF16)),
            in_specs=[vmem, vmem],
            out_specs=(any_spec,) * 4,
            scratch_shapes=[pltpu.SemaphoreType.DMA((2,))],
            compiler_params=pltpu.CompilerParams(vmem_limit_bytes=4 * 1024 * 1024),
            name="write_log_probs",
        )(z, fin)
        return log_norm.reshape(rows), entropy.reshape(rows), target_logp.reshape(rows), log_probs

    return jax.shard_map(
        device_step,
        mesh=mesh,
        in_specs=(P("dp", None), P(None, "tp"), P(None, "tp"), P("tp", None), P(None),
                  P(None, "tp"), P("dp"), P("dp")),
        out_specs=(P("dp"), P("dp"), P("dp"), P("dp", None)),
        check_vma=False,
    )
```
